32 devices in a mesh: tx: 4 (over z), ty: 4 (over y, core), gz: 2 (over x).
Axes of the slice: x: 2, y: 2, z: 4, core: 2. Of those that a mesh axis runs over, the one named last changes fastest.
Arguments:
- design: float32 [128, 1024, 256], P('tx', 'ty', 'gz'), may hold values from 0.05 to 0.95
- forward_edges: float32 [2, 12, 65536], P(None, None, ('tx', 'ty', 'gz')), may hold values from -6 to 6
- adjoint_edges: float32 [2, 12, 65536], P(None, None, ('tx', 'ty', 'gz')), may hold values from -6 to 6
- edge_basis: float32 [24, 12], replicated, may hold values from -1.75 to 1.75
- quad_weights: float32 [8], replicated, may hold values from 0.05 to 0.25
- slot_weights: bfloat16 [512, 16, 128], P(('tx', 'ty', 'gz')), may hold values from 0.049804688 to 1
- slot_elements: int32 [512, 16], P(('tx', 'ty', 'gz')), may hold values from 0 to 2047
- slot_blocks: int32 [512, 16], P(('tx', 'ty', 'gz')), may hold values from 0 to 8191
- slot_counts: int32 [32, 16], P(('tx', 'ty', 'gz')), may hold values from 1 to 16, 128 in all within a row
Outputs:
- projected: float32 [128, 1024, 256], P('tx', 'ty', 'gz')
- element_density: float32 [65536], P(('tx', 'ty', 'gz'))
The draws below stay inside these ranges and needn't reach their ends.
Inputs may be any that keep to these rules, and one draw needn't show every extreme that they name: `slot_counts`: in every row of each partition the counts sum to 16 * 16 // 2 and the largest equals 16.
All inputs are finite; a program needn't handle non-finite values.
Results may differ from the reference program's by a relative error of at most 0.00055.
Values may be sent and summed in bfloat16 or wider, within the bound.
No kernel may reach another device: no remote copies, remote signals or barrier semaphores. Data moves between devices by JAX's collectives and lax.ppermute only.
A program may use at most 128 MiB of HBM per device.

```python
import math
import jax
import jax.numpy as jnp
import numpy as np
from jax import lax

VX = 32
VY = 256
VZ = 128
E_DEV = 2048
CAP = 16
QUAD = 8
EDGES = 12
RADIUS = 8
BLOCK_VOX = 128
TILES = 16
BLOCKS_DEV = 8192
NX = 128
NY = 1024
NZ = 256
ELEMS = 65536
SLOT_ROWS = 512
N_TX = 4
N_TY = 4
N_GZ = 2
DEVICES = 32


def with_ends(drawn, rng, low, high):
    index_at = [jax.random.randint(jax.random.fold_in(rng, axis), (), 0, length) for axis, length in enumerate(drawn.shape)]
    widest = drawn.shape.index(max(drawn.shape))
    next_to = index_at[:widest] + [(index_at[widest] + 1) % drawn.shape[widest]] + index_at[widest + 1:]
    return drawn.at[tuple(index_at)].set(low).at[tuple(next_to)].set(high)


def block_scale(rng, extent, split, least, largest):
    loudness = 1.0
    for position, blocks in split:
        heights = jax.random.uniform(jax.random.fold_in(jax.random.fold_in(rng, 6), position), (blocks,), jnp.float32, least / len(split), largest / len(split))
        loudness = loudness * jnp.repeat(jnp.exp(heights), extent[position] // blocks).reshape((-1,) + (1,) * (len(extent) - 1 - position))
    return loudness


def length_profile(amount, total, reach, skew):
    portions = [(1 << 20) // math.isqrt(rank ** skew) + 1 for rank in range(2, amount + 1)]
    rest, holding = total - reach - (amount - 1), [1] * (amount - 1)
    while rest > 0:
        free = [i for i in range(amount - 1) if holding[i] < reach]
        mass, left = sum([portions[i] for i in free]), rest
        for i in free:
            more = min(reach - holding[i], max(1, left * portions[i] // mass), rest)
            holding[i] = holding[i] + more
            rest = rest - more
    return np.array([reach] + holding)


def ragged_sizes(rng, number_of, total, limit, lean):
    if number_of == 2:
        one = jax.random.randint(rng, (), max(1, total - limit), min(limit, total - 1) + 1)
        return jnp.stack([one, total - one])
    lengths = jnp.asarray(length_profile(number_of, total, limit, lean), jnp.int32)
    couples = (number_of - 1) // 2
    donor, receiver = lengths[1:1 + 2 * couples:2], lengths[2:2 + 2 * couples:2]
    margin = jnp.minimum(donor - 1, limit - receiver)
    moved = jax.random.randint(jax.random.fold_in(rng, 1), (couples,), 0, 1 << 20) % (margin + 1)
    lengths = lengths.at[1:1 + 2 * couples:2].set(donor - moved).at[2:2 + 2 * couples:2].set(receiver + moved)
    return lengths[jax.random.permutation(jax.random.fold_in(rng, 2), number_of)]


def centred(key, dims, spread, bound, shards=(), held_as=jnp.bfloat16):
    factor_of = block_scale(key, dims, shards, -0.22, 0.18) if shards else 1.0
    drawn = jax.random.normal(key, dims, jnp.float32) * spread * factor_of
    return jnp.minimum(jnp.maximum(drawn, -bound), bound).astype(held_as)


def setup_inputs(seed: int = 0) -> dict:
    key_of = jax.random.split(jax.random.key(seed), 10)
    design = jnp.clip(0.05 + 0.9 * jax.random.uniform(key_of[0], (NX, NY, NZ), jnp.float32) ** block_scale(key_of[0], (NX, NY, NZ), ((0, 4), (1, 4), (2, 2)), -0.2, 0.2), 0.05, 0.95)
    forward_edges = centred(key_of[1], (2, EDGES, ELEMS), 1.0, 6.0, ((2, 32),), jnp.float32)
    adjoint_edges = centred(key_of[2], (2, EDGES, ELEMS), 1.0, 6.0, ((2, 32),), jnp.float32)
    edge_basis = centred(key_of[3], (3 * QUAD, EDGES), EDGES ** -0.5, 1.75, (), jnp.float32)
    quad_weights = jnp.clip(jax.random.uniform(key_of[4], (QUAD,), jnp.float32, 0.05, 0.25), 0.05, 0.25)
    slot_weights = jnp.clip(0.049804688 + 0.9501953 * jax.random.uniform(key_of[5], (SLOT_ROWS, CAP, BLOCK_VOX), jnp.float32) ** block_scale(key_of[5], (SLOT_ROWS, CAP, BLOCK_VOX), ((0, 32),), -0.2, 0.2), 0.049804688, 1.0).astype(jnp.bfloat16)
    slot_elements = with_ends(jax.random.randint(key_of[6], (SLOT_ROWS, CAP), 0, E_DEV), jax.random.fold_in(key_of[6], 1), 0, E_DEV - 1).astype(jnp.int32)
    slot_blocks = with_ends(jax.random.randint(key_of[7], (SLOT_ROWS, CAP), 0, BLOCKS_DEV), jax.random.fold_in(key_of[7], 1), 0, BLOCKS_DEV - 1).astype(jnp.int32)
    slot_counts = jax.vmap(lambda own: ragged_sizes(own, TILES, TILES * CAP // 2, CAP, 2))(jax.random.split(key_of[8], DEVICES)).reshape((DEVICES, TILES)).astype(jnp.int32)
    return dict(design=design, forward_edges=forward_edges, adjoint_edges=adjoint_edges, edge_basis=edge_basis, quad_weights=quad_weights, slot_weights=slot_weights, slot_elements=slot_elements, slot_blocks=slot_blocks, slot_counts=slot_counts)


def filter_kernel(radius):
    values = [float(radius + 1 - abs(offset)) for offset in range(-radius, radius + 1)]
    total = sum(values)
    return [value / total for value in values]


def along(padded, kernel, dimension, length):
    summed = kernel[0] * lax.slice_in_dim(padded, 0, length, axis=dimension)
    for offset in range(1, len(kernel)):
        summed = summed + kernel[offset] * lax.slice_in_dim(padded, offset, offset + length, axis=dimension)
    return summed


def project(filtered):
    sharp = 8.0
    middle = 0.5
    span_total = math.tanh(sharp * middle) + math.tanh(sharp * (1.0 - middle))
    return (math.tanh(sharp * middle) + jnp.tanh(sharp * (filtered - middle))) / span_total


def sensitivity(edge_basis, quad_weights, forward_edges, adjoint_edges):
    highest = lax.Precision.HIGHEST
    forward_field = jnp.einsum("qk,rke->rqe", edge_basis, forward_edges, precision=highest)
    adjoint_field = jnp.einsum("qk,rke->rqe", edge_basis, adjoint_edges, precision=highest)
    product = forward_field[0] * adjoint_field[0] - forward_field[1] * adjoint_field[1]
    points = quad_weights.shape[0]
    product = product.reshape(3, points, -1).sum(axis=0)
    return jnp.dot(quad_weights, product, precision=highest)


def reference(design, forward_edges, adjoint_edges, edge_basis, quad_weights, slot_weights, slot_elements, slot_blocks, slot_counts):
    device_count = N_TX * N_TY * N_GZ
    tile_count = N_TX * N_TY
    sensitivities = sensitivity(edge_basis, quad_weights, forward_edges, adjoint_edges)
    live_slots = jnp.arange(CAP, dtype=jnp.int32)[None, None, :] < slot_counts[:, :, None]
    owner_index = jnp.arange(device_count, dtype=jnp.int32)[:, None, None]
    elements = slot_elements.reshape(device_count, tile_count, CAP) + owner_index * E_DEV
    slot_value = jnp.where(live_slots, sensitivities[elements], jnp.float32(0.0)).astype(jnp.bfloat16)
    target = jnp.arange(tile_count, dtype=jnp.int32)[None, :, None]
    block_index = (target * N_GZ + owner_index % N_GZ) * BLOCKS_DEV + slot_blocks.reshape(device_count, tile_count, CAP)
    weights = slot_weights.astype(jnp.float32).reshape(device_count, tile_count, CAP, BLOCK_VOX)
    deposits = weights * slot_value.astype(jnp.float32)[..., None]
    gradient_blocks = jnp.zeros((tile_count * N_GZ * BLOCKS_DEV, BLOCK_VOX), jnp.float32)
    gradient_blocks = gradient_blocks.at[block_index.reshape(-1)].add(deposits.reshape(-1, BLOCK_VOX))
    shaped = gradient_blocks.reshape(N_TX, N_TY, N_GZ, VX, VY, VZ)
    gradient = shaped.transpose(0, 3, 1, 4, 2, 5).reshape(NX, NY, NZ)
    updated = jnp.clip(design - 0.5 * gradient, 0.0, 1.0)
    kernel = filter_kernel(RADIUS)
    padded = jnp.pad(updated, ((RADIUS, RADIUS), (0, 0), (0, 0)), mode="wrap")
    smoothed = along(padded, kernel, 0, NX)
    padded = jnp.pad(smoothed, ((0, 0), (RADIUS, RADIUS), (0, 0)), mode="wrap")
    smoothed = along(padded, kernel, 1, NY)
    padded = jnp.pad(smoothed, ((0, 0), (0, 0), (RADIUS, RADIUS)))
    smoothed = along(padded, kernel, 2, NZ)
    normaliser = along(jnp.pad(jnp.ones((NZ,), jnp.float32), (RADIUS, RADIUS)), kernel, 0, NZ)
    projected = project(smoothed / normaliser[None, None, :])
    grouped = projected.reshape(N_TX, VX, N_TY, VY, N_GZ, VZ)
    projected_blocks = grouped.transpose(0, 2, 4, 1, 3, 5).reshape(-1, BLOCK_VOX)
    picked = projected_blocks[block_index]
    ratios = jnp.sum(weights * picked, axis=-1) / jnp.sum(weights, axis=-1)
    element_density = jnp.zeros((device_count * E_DEV,), jnp.float32)
    element_density = element_density.at[elements.reshape(-1)].add(jnp.where(live_slots, ratios, jnp.float32(0.0)).reshape(-1))
    return projected, element_density
```

```python
import functools
import math

import jax
import jax.numpy as jnp
from jax import lax
from jax.experimental import pallas as pl
from jax.experimental.pallas import tpu as pltpu
from jax.sharding import PartitionSpec as P

RADIUS = 8
LANES = 128
TAPS = RADIUS + 1
F32 = jnp.float32
BF16 = jnp.bfloat16
SMEM = pltpu.SMEM
VMEM = pltpu.VMEM


def iota(shape, dim):
    return lax.broadcasted_iota(jnp.int32, shape, dim)


def cone(distance):
    return jnp.maximum(TAPS - jnp.abs(distance), 0).astype(F32)


def halves(x):
    high = x.astype(BF16)
    return high, (x - high.astype(F32)).astype(BF16)


def dot(a, b, contract=((1,), (0,))):
    return lax.dot_general(a, b, (contract, ((), ())), preferred_element_type=F32)


def sensitivity(edge_basis, quad_weights, forward_edges, adjoint_edges):
    highest = lax.Precision.HIGHEST
    forward_field = jnp.einsum("qk,rke->rqe", edge_basis, forward_edges, precision=highest)
    adjoint_field = jnp.einsum("qk,rke->rqe", edge_basis, adjoint_edges, precision=highest)
    product = forward_field[0] * adjoint_field[0] - forward_field[1] * adjoint_field[1]
    points = quad_weights.shape[0]
    product = product.reshape(3, points, -1).sum(axis=0)
    return jnp.dot(quad_weights, product, precision=highest)


def deposit_kernel(
    cells_y, slots, rows_ref, vals_ref, zoff_ref, design_ref, low_ref, high_ref, pay_ref,
    smooth_ref, rim_ref, grid_ref,
):
    cells_x = design_ref.shape[0]
    partners = pay_ref.shape[0]

    @pl.loop(0, RADIUS)
    def _(x):
        grid_ref[pl.ds(x * cells_y, cells_y), :] = low_ref[x].astype(F32)
        grid_ref[pl.ds((x + RADIUS + cells_x) * cells_y, cells_y), :] = high_ref[x].astype(F32)

    @pl.loop(0, cells_x)
    def _(x):
        grid_ref[pl.ds((x + RADIUS) * cells_y, cells_y), :] = design_ref[x] - 0.5

    @pl.loop(0, partners)
    def _(p):
        for s in range(slots):
            row = rows_ref[p * slots + s]

            @pl.when(row >= 0)
            def _():
                amount = vals_ref[p * slots + s] * pay_ref[p, s : s + 1, :].astype(F32)
                grid_ref[pl.ds(row, 1), :] = grid_ref[pl.ds(row, 1), :] + amount

    @pl.loop(0, cells_y // 8)
    def _(j):
        def plane(e):
            u = grid_ref[pl.ds(pl.multiple_of(e * cells_y + j * 8, 8), 8), :]
            return jnp.clip(u, -0.5, 0.5)

        u = [plane(e) for e in range(cells_x + 2 * RADIUS)]
        box = [functools.reduce(lambda a, b: a + b, u[:TAPS])]
        for k in range(cells_x + RADIUS - 1):
            box.append(box[-1] + (u[k + TAPS] - u[k]))
        total = functools.reduce(lambda a, b: a + b, box[:TAPS])
        for i in range(cells_x):
            smooth_ref[i, pl.ds(pl.multiple_of(j * 8, 8), 8), :] = total
            if i + 1 < cells_x:
                total = total + (box[i + TAPS] - box[i])

    pick = (iota((RADIUS, LANES), 1) == iota((RADIUS, LANES), 0) + zoff_ref[0]).astype(F32)
    pick = pick.astype(BF16)

    @pl.loop(0, cells_x)
    def _(x):
        rim = dot(pick, smooth_ref[x].astype(BF16), ((1,), (1,)))
        rim_ref[x] = rim.astype(BF16)


def z_kernel(zoff_ref, smooth_ref, rim_ref, out_ref, first_ref, last_ref):
    cells_x, cells_y, cells_z = smooth_ref.shape
    weights = cone(iota((cells_z, cells_z), 0) - iota((cells_z, cells_z), 1)).astype(BF16)
    weights = jnp.concatenate([weights, weights], axis=0)
    side = iota((RADIUS, cells_z), 0) + zoff_ref[1] - iota((RADIUS, cells_z), 1)
    side = (cone(side) * zoff_ref[2].astype(F32)).astype(BF16)

    @pl.loop(0, cells_x)
    def _(x):
        pair = jnp.concatenate(halves(smooth_ref[x]), axis=1)
        value = dot(pair, weights) + dot(rim_ref[x], side, ((0,), (0,)))
        out_ref[x] = value
        first_ref[x] = value[:RADIUS].astype(BF16)
        last_ref[x] = value[cells_y - RADIUS :].astype(BF16)


def y_kernel(
    scale_total, rows_ref, zoff_ref, h_ref, before_ref, after_ref, pay_ref, out_ref, ratio_ref,
    proj_ref, picked_ref,
):
    planes, cells_y, cells_z = h_ref.shape
    partners, capacity, _ = pay_ref.shape
    step = pl.program_id(0)
    weights = cone(iota((cells_y, cells_y), 0) - iota((cells_y, cells_y), 1)).astype(BF16)
    column = iota((cells_y, 2 * RADIUS), 1)
    place = jnp.where(column < RADIUS, column - RADIUS, column - RADIUS + cells_y)
    edge = cone(place - iota((cells_y, 2 * RADIUS), 0)).astype(BF16)
    z = iota((1, cells_z), 1) + zoff_ref[3]
    inside = jnp.zeros((1, cells_z), F32)
    for offset in range(-RADIUS, RADIUS + 1):
        good = (z + offset >= 0) & (z + offset < zoff_ref[4])
        inside = inside + jnp.where(good, float(TAPS - abs(offset)), 0.0)
    scale = 8.0 / (scale_total * inside)
    top = math.tanh(4.0)
    for x in range(planes):
        pair = jnp.concatenate(halves(h_ref[x]), axis=1)
        both = dot(weights, pair)
        value = both[:, :cells_z] + both[:, cells_z:]
        rims = jnp.concatenate([before_ref[x].astype(F32), after_ref[x].astype(F32)], axis=0)
        value = value + dot(edge, rims.astype(BF16))
        value = (top + jnp.tanh(value * scale)) * (1.0 / (2.0 * top))
        out_ref[x] = value
        proj_ref[pl.ds(pl.multiple_of((step * planes + x) * cells_y, 8), cells_y), :] = value

    @pl.when(step == pl.num_programs(0) - 1)
    def _():
        @pl.loop(0, partners)
        def _(p):
            for s in range(capacity):
                row = rows_ref[p * capacity + s]
                picked_ref[pl.ds(p * capacity + s, 1), :] = proj_ref[pl.ds(row, 1), :]

        ones = jnp.ones((8, cells_z), BF16)
        group = LANES // capacity

        @pl.loop(0, partners * capacity // LANES)
        def _(c):
            w = pay_ref[pl.ds(c * group, group)].reshape(LANES, cells_z)
            picked = picked_ref[pl.ds(pl.multiple_of(c * LANES, LANES), LANES), :]
            high, low = halves(w.astype(F32) * picked)
            nt = ((1,), (1,))
            total = dot(ones, high, nt) + dot(ones, low, nt)
            ratio_ref[pl.ds(c, 1), :] = (total / dot(ones, w, nt))[:1]


def back_kernel(counts_ref, elements_ref, ratio_ref, out_ref):
    tiles, capacity = elements_ref.shape
    high_count = out_ref.shape[0]
    total = jnp.zeros(out_ref.shape, F32)
    for t in range(tiles):
        element = elements_ref[pl.ds(t, 1), :]
        live = iota((1, capacity), 1) < counts_ref[0, t]
        ratio = jnp.where(live, ratio_ref[pl.ds(t, 1), :], 0.0)
        lane = (iota((LANES, capacity), 0) == (element & (LANES - 1))).astype(F32).astype(BF16)
        spread = jnp.where(iota((high_count, capacity), 0) == element // LANES, ratio, 0.0)
        high, low = halves(spread)
        nt = ((1,), (1,))
        total = total + (dot(high, lane, nt) + dot(low, lane, nt))
    out_ref[...] = total


def body(
    design,
    forward_edges,
    adjoint_edges,
    edge_basis,
    quad_weights,
    slot_weights,
    slot_elements,
    slot_blocks,
    slot_counts,
):
    cells_x, cells_y, cells_z = design.shape
    tiles, capacity = slot_elements.shape
    n_tx, n_ty, n_gz = (lax.axis_size(a) for a in ("tx", "ty", "gz"))
    if cells_z != LANES or cells_y > 256 or n_gz != 2:
        raise NotImplementedError
    gz = lax.axis_index("gz")
    up = [(i, (i + 1) % n_tx) for i in range(n_tx)]
    down = [(t, s) for s, t in up]
    low = lax.ppermute((design[-RADIUS:] - 0.5).astype(BF16), "tx", up)
    high = lax.ppermute((design[:RADIUS] - 0.5).astype(BF16), "tx", down)

    sens = sensitivity(edge_basis, quad_weights, forward_edges, adjoint_edges)
    live = jnp.arange(capacity, dtype=jnp.int32)[None, :] < slot_counts[0][:, None]
    value = jnp.where(live, sens[slot_elements], F32(0.0)).astype(BF16)
    value = (value.astype(F32) * -0.5).astype(BF16)
    plane = (slot_blocks // cells_y + RADIUS).astype(F32)
    line = (slot_blocks % cells_y).astype(F32).astype(BF16)

    def shifted(a, d):
        a = a.reshape((n_tx, n_ty) + a.shape[1:])
        return jnp.roll(a, -d, axis=0).reshape((tiles,) + a.shape[2:])

    offsets = (0, -1, 1)
    rows3 = jnp.concatenate([shifted(slot_weights, d) for d in offsets], axis=1)
    planes3 = jnp.concatenate([shifted(plane, d) + float(cells_x * d) for d in offsets], axis=1)
    lines3 = jnp.concatenate([shifted(line, d) for d in offsets], axis=1)
    values3 = jnp.concatenate([shifted(value, d) for d in offsets], axis=1)
    slots = 3 * capacity
    meta = jnp.stack([planes3.astype(BF16), lines3, values3], axis=1)
    meta = jnp.pad(meta, ((0, 0), (0, 5), (0, LANES - slots)))
    payload = jnp.concatenate([rows3, meta], axis=1)
    arrived = lax.all_to_all(payload, ("tx", "ty"), split_axis=0, concat_axis=0, tiled=True)
    meta = arrived[:, slots : slots + 3, :slots].astype(F32)
    rows = meta[:, 0] * float(cells_y) + meta[:, 1]
    rows = rows.astype(jnp.int32)
    vals = meta[:, 2]
    ext_rows = (cells_x + 2 * RADIUS) * cells_y
    used = (rows >= 0) & (rows < ext_rows) & (vals != 0.0)
    rows_used = jnp.where(used, rows, -1).reshape(-1)
    rows_own = (rows[:, :capacity] - RADIUS * cells_y).reshape(-1)

    zoff = jnp.stack(
        [
            jnp.where(gz == 0, cells_z - RADIUS, 0),
            jnp.where(gz == 0, cells_z, -RADIUS),
            jnp.int32(1),
            gz * cells_z,
            jnp.int32(n_gz * cells_z),
        ]
    ).astype(jnp.int32)

    whole = pl.BlockSpec(memory_space=VMEM)
    scalars = pl.BlockSpec(memory_space=SMEM)
    smooth, rim = pl.pallas_call(
        functools.partial(deposit_kernel, cells_y, slots),
        out_shape=(
            jax.ShapeDtypeStruct((cells_x, cells_y, cells_z), F32),
            jax.ShapeDtypeStruct((cells_x, RADIUS, cells_y), BF16),
        ),
        in_specs=[scalars] * 3 + [whole] * 4,
        out_specs=(whole, whole),
        scratch_shapes=[VMEM((ext_rows, cells_z), F32)],
        name="deposit",
    )(rows_used, vals.reshape(-1), zoff, design, low, high, arrived)

    rim = lax.ppermute(rim, "gz", [(0, 1), (1, 0)])
    edge = jax.ShapeDtypeStruct((cells_x, RADIUS, cells_z), BF16)
    h, first, last = pl.pallas_call(
        z_kernel,
        out_shape=(jax.ShapeDtypeStruct((cells_x, cells_y, cells_z), F32), edge, edge),
        in_specs=[scalars, whole, whole],
        out_specs=(whole, whole, whole),
        name="smooth_z",
    )(zoff, smooth, rim)

    up = [(i, (i + 1) % n_ty) for i in range(n_ty)]
    down = [(t, s) for s, t in up]
    before = lax.ppermute(last, "ty", up)
    after = lax.ppermute(first, "ty", down)

    step = 4
    block = lambda *shape: pl.BlockSpec(shape, lambda i: (i, 0, 0))
    projected, ratios = pl.pallas_call(
        functools.partial(y_kernel, float(TAPS**4)),
        grid=(cells_x // step,),
        out_shape=(
            jax.ShapeDtypeStruct((cells_x, cells_y, cells_z), F32),
            jax.ShapeDtypeStruct((tiles * capacity // LANES, LANES), F32),
        ),
        in_specs=[
            scalars,
            scalars,
            block(step, cells_y, cells_z),
            block(step, RADIUS, cells_z),
            block(step, RADIUS, cells_z),
            pl.BlockSpec((tiles, capacity, cells_z), lambda i: (0, 0, 0)),
        ],
        out_specs=(
            block(step, cells_y, cells_z),
            pl.BlockSpec((tiles * capacity // LANES, LANES), lambda i: (0, 0)),
        ),
        scratch_shapes=[
            VMEM((cells_x * cells_y, cells_z), F32),
            VMEM((tiles * capacity, cells_z), F32),
        ],
        name="smooth_y",
    )(rows_own, zoff, h, before, after, arrived)

    ratios = ratios.reshape(tiles, capacity)
    ratios = lax.all_to_all(ratios, ("tx", "ty"), split_axis=0, concat_axis=0, tiled=True)
    elements = forward_edges.shape[2]
    density = pl.pallas_call(
        back_kernel,
        out_shape=jax.ShapeDtypeStruct((elements // LANES, LANES), F32),
        in_specs=[scalars, whole, whole],
        out_specs=whole,
        name="to_elements",
    )(slot_counts, slot_elements, ratios)
    return projected, density.reshape(elements)


def solution(mesh):
    in_specs = (
        P("tx", "ty", "gz"),
        P(None, None, ("tx", "ty", "gz")),
        P(None, None, ("tx", "ty", "gz")),
        P(),
        P(),
        P(("tx", "ty", "gz"), None, None),
        P(("tx", "ty", "gz"), None),
        P(("tx", "ty", "gz"), None),
        P(("tx", "ty", "gz"), None),
    )
    out_specs = (P("tx", "ty", "gz"), P(("tx", "ty", "gz")))
    return jax.shard_map(body, mesh=mesh, in_specs=in_specs, out_specs=out_specs, check_vma=False)
```

```python
import functools
import math

import jax
import jax.numpy as jnp
from jax import lax
from jax.experimental import pallas as pl
from jax.experimental.pallas import tpu as pltpu
from jax.sharding import PartitionSpec as P

RADIUS = 8
LANES = 128
TAPS = RADIUS + 1
F32 = jnp.float32
BF16 = jnp.bfloat16
SMEM = pltpu.SMEM
VMEM = pltpu.VMEM
NT = ((1,), (1,))
TN = ((0,), (0,))


def iota(shape, dim):
    return lax.broadcasted_iota(jnp.int32, shape, dim)


def onehot(mask):
    return mask.astype(F32).astype(BF16)


def cone(distance):
    return jnp.maximum(TAPS - jnp.abs(distance), 0).astype(F32).astype(BF16)


def halves(x):
    high = x.astype(BF16)
    return high, (x - high.astype(F32)).astype(BF16)


def dot(a, b, contract=((1,), (0,)), precision=None):
    return lax.dot_general(
        a, b, (contract, ((), ())), preferred_element_type=F32, precision=precision
    )


def picker(first):
    return onehot(iota((RADIUS, LANES), 1) == iota((RADIUS, LANES), 0) + first)


def running(planes, length):
    add = lambda a, b: a + b
    box = [functools.reduce(add, planes[:TAPS])]
    for k in range(length + RADIUS - 1):
        box.append(box[-1] + (planes[k + TAPS] - planes[k]))
    total = functools.reduce(add, box[:TAPS])
    out = [total]
    for i in range(length - 1):
        total = total + (box[i + TAPS] - box[i])
        out.append(total)
    return out


def clipped(x):
    return jnp.clip(x, -0.5, 0.5)


def pack_kernel(
    n_ty, counts_ref, quad_ref, zoff_ref, basis_ref, forward_ref, adjoint_ref, weights_ref,
    elements_ref, blocks_ref, design_ref, pay_ref, up_edge_ref, down_edge_ref, up_ref, down_ref,
    strip_ref, code_ref, sem,
):
    cells_x, cells_y, _ = design_ref.shape
    tiles, capacity = elements_ref.shape
    points = quad_ref.shape[0]
    highest = lax.Precision.HIGHEST
    copies = [
        pltpu.make_async_copy(
            design_ref.at[pl.ds(start, RADIUS)], strip_ref.at[pl.ds(side * RADIUS, RADIUS)],
            sem.at[side],
        )
        for side, start in enumerate((0, cells_x - RADIUS))
    ]
    for copy in copies:
        copy.start()

    terms, edges = 2 * forward_ref.shape[0], forward_ref.shape[0]
    point = iota((1, 3 * points), 1) % points
    quad = jnp.zeros((1, 3 * points), F32)
    for q in range(points):
        quad = quad + jnp.where(point == q, quad_ref[q], 0.0)
    twice = (iota((terms, edges), 0) // 2 == iota((terms, edges), 1)).astype(F32)
    basis = dot(twice, basis_ref[...], precision=highest)
    gram = dot(basis * quad, basis, NT, precision=highest)
    row, column = iota((terms, terms), 0), iota((terms, terms), 1)
    gram = jnp.where(row % 2 == 0, gram, -gram)
    gram = jnp.where(row % 2 == column % 2, gram, 0.0)
    adjoint = jnp.concatenate([adjoint_ref[k] for k in range(edges)], axis=0)
    forward = jnp.concatenate([forward_ref[k] for k in range(edges)], axis=0)
    sens = jnp.sum(forward * dot(gram, adjoint, precision=highest), axis=0, keepdims=True)
    groups = sens.shape[1] // LANES
    sens = jnp.concatenate([sens[:, g * LANES : (g + 1) * LANES] for g in range(groups)], axis=0)
    first, rest = halves(sens)
    second, third = halves(sens - first.astype(F32))
    parts = jnp.concatenate([first, second, third], axis=0)

    element, block = elements_ref[...], blocks_ref[...]
    codes = [
        element // LANES,
        element % LANES,
        block // cells_y + RADIUS,
        block % cells_y,
    ]
    place = iota((capacity, LANES), 1) - iota((capacity, LANES), 0)
    for index, code in enumerate(codes):
        code = code.astype(F32).astype(BF16)
        total = jnp.zeros((tiles, LANES), F32)
        for order, d in enumerate((0, -1, 1)):
            moved = dot(code, onehot(place == order * capacity))
            shift = (d * n_ty) % tiles
            if shift:
                moved = jnp.concatenate([moved[shift:], moved[:shift]], axis=0)
            if index == 2 and d:
                group = iota((tiles, LANES), 1) // capacity
                moved = moved + jnp.where(group == order, float(d * cells_x), 0.0)
            total = total + moved
        code_ref[index] = total

    @pl.loop(0, tiles, unroll=min(tiles, 16))
    def _(t):
        high, low, plane, line = (code_ref[index, pl.ds(t, 1), :] for index in range(4))
        lane = iota((1, LANES), 1)
        live = jnp.zeros((1, LANES), jnp.bool_)
        sources = []
        for order, d in enumerate((0, -1, 1)):
            source = lax.rem(t + (d * n_ty) % tiles, tiles)
            sources.append(source)
            at = lane - order * capacity
            live = live | ((at >= 0) & (at < capacity) & (at < counts_ref[0, source]))
        hit = onehot(iota((LANES, LANES), 0).astype(F32) == low)
        found = dot(parts, hit)
        found = (found[:groups] + found[groups : 2 * groups]) + found[2 * groups :]
        mine = iota((groups, LANES), 0).astype(F32) == high
        value = jnp.sum(jnp.where(mine, found, 0.0), axis=0, keepdims=True)
        value = jnp.where(live, value, 0.0).astype(BF16).astype(F32) * -0.5
        kind = iota((8, LANES), 0)
        meta = jnp.where(kind == 0, plane, jnp.where(kind == 1, line, value))
        meta = jnp.where(kind < 3, meta, 0.0)
        for order, source in enumerate(sources):
            pay_ref[t, order * capacity : (order + 1) * capacity, :] = weights_ref[source]
        pay_ref[t, 3 * capacity :, :] = meta.astype(BF16)

    pick = picker(zoff_ref[0])
    for side, (edge_ref, main_ref) in enumerate(((down_edge_ref, down_ref), (up_edge_ref, up_ref))):
        copies[side].wait()

        @pl.loop(0, RADIUS, unroll=2)
        def _(p):
            plane = strip_ref[side * RADIUS + p] - 0.5
            main_ref[p] = plane[RADIUS : cells_y - RADIUS].astype(BF16)
            edge_ref[p, :RADIUS] = plane[:RADIUS].astype(BF16)
            edge_ref[p, RADIUS : 2 * RADIUS] = plane[cells_y - RADIUS :].astype(BF16)
            flipped = dot(pick, plane.astype(BF16), NT).astype(BF16)
            for k in range(cells_y // LANES):
                start = (2 + k) * RADIUS
                edge_ref[p, start : start + RADIUS] = flipped[:, k * LANES : (k + 1) * LANES]


def deposit_kernel(
    cells_y, slots, rows_ref, vals_ref, zoff_ref, design_ref, low_ref, high_ref, pay_ref,
    grid_ref, rows_out_ref, rim_ref, flip_ref, sem,
):
    cells_x = design_ref.shape[0] // cells_y
    partners = pay_ref.shape[0]
    rim = RADIUS * cells_y
    own = cells_x * cells_y
    copy = pltpu.make_async_copy(design_ref, grid_ref.at[pl.ds(rim, own)], sem)
    copy.start()

    zeros = jnp.zeros((cells_y, LANES), F32)
    for p in range(RADIUS):
        grid_ref[p * cells_y : (p + 1) * cells_y, :] = zeros
        grid_ref[rim + own + p * cells_y : rim + own + (p + 1) * cells_y, :] = zeros
    copy.wait()

    @pl.loop(0, partners)
    def _(p):
        for s in range(slots):
            row = rows_ref[p * slots + s]

            @pl.when(row >= 0)
            def _():
                amount = vals_ref[p * slots + s] * pay_ref[p, s : s + 1, :].astype(F32)
                grid_ref[pl.ds(row, 1), :] = grid_ref[pl.ds(row, 1), :] + amount

    total = cells_x + 2 * RADIUS
    pick = picker(zoff_ref[0])

    @pl.loop(0, cells_x, unroll=4)
    def _(x):
        plane = clipped(grid_ref[pl.ds(rim + x * cells_y, cells_y), :] - 0.5)
        flip_ref[x + RADIUS] = dot(pick, plane.astype(BF16), NT)

    for source_ref, base in ((low_ref, 0), (high_ref, RADIUS + cells_x)):
        @pl.loop(0, RADIUS, unroll=4)
        def _(p):
            plane = grid_ref[pl.ds((base + p) * cells_y, cells_y), :]
            deposited = dot(pick, plane.astype(BF16), NT)
            raw = jnp.concatenate(
                [
                    source_ref[p, (2 + k) * RADIUS : (3 + k) * RADIUS].astype(F32)
                    for k in range(cells_y // LANES)
                ],
                axis=1,
            )
            flip_ref[base + p] = clipped(raw + deposited)

    for source_ref, base in ((low_ref, 0), (high_ref, RADIUS + cells_x)):
        for p in range(RADIUS):
            for k, start in enumerate((0, cells_y - RADIUS)):
                at = (base + p) * cells_y + start
                edge = source_ref[p, k * RADIUS : (k + 1) * RADIUS].astype(F32)
                grid_ref[at : at + RADIUS, :] = grid_ref[at : at + RADIUS, :] + edge

    for k, start in enumerate((0, cells_y - RADIUS)):
        planes = []
        for e in range(total):
            at = e * cells_y + start
            bias = 0.5 if RADIUS <= e < RADIUS + cells_x else 0.0
            planes.append(clipped(grid_ref[at : at + RADIUS, :] - bias))
        for i, value in enumerate(running(planes, cells_x)):
            rows_out_ref[i, k * RADIUS : (k + 1) * RADIUS, :] = value

    for i, value in enumerate(running([flip_ref[e] for e in range(total)], cells_x)):
        rim_ref[i] = value.astype(BF16)


def edge_kernel(zoff_ref, rows_ref, rim_ref, first_ref, last_ref):
    cells_x, double, cells_z = rows_ref.shape
    cells_y = rim_ref.shape[2]
    weights = cone(iota((cells_z, cells_z), 0) - iota((cells_z, cells_z), 1))
    weights = jnp.concatenate([weights, weights], axis=0)
    side = cone(iota((RADIUS, cells_z), 0) + zoff_ref[1] - iota((RADIUS, cells_z), 1))
    rows = rows_ref[...].reshape(cells_x * double, cells_z)
    value = dot(jnp.concatenate(halves(rows), axis=1), weights)
    for x in range(cells_x):
        for k, out_ref in enumerate((first_ref, last_ref)):
            start = 0 if k == 0 else cells_y - LANES
            shift = 0 if k == 0 else LANES - RADIUS
            rim = rim_ref[x, :, start : start + LANES][:, shift : shift + RADIUS]
            at = x * double + k * RADIUS
            out_ref[x] = (value[at : at + RADIUS] + dot(rim, side, TN)).astype(BF16)


def finish_kernel(
    scale_total, rows_ref, zoff_ref, grid_ref, low_ref, high_ref, rim_ref, before_ref, after_ref,
    pay_ref, out_ref, ratio_ref, rims_ref, smooth_ref, proj_ref, picked_ref, sem,
):
    cells_x, _, cells_y = rim_ref.shape
    cells_z = out_ref.shape[1]
    partners = pay_ref.shape[0]
    capacity = picked_ref.shape[0] // partners
    total = cells_x + 2 * RADIUS
    inner = cells_y - 2 * RADIUS
    chunk = 16

    for source_ref, base, into in ((low_ref, 0, 0), (high_ref, RADIUS + cells_x, RADIUS)):
        @pl.loop(0, RADIUS)
        def _(p):
            at = pl.multiple_of((base + p) * cells_y, 8)
            to = pl.multiple_of((into + p) * cells_y, 8)
            main = grid_ref[pl.ds(at + RADIUS, inner), :] + source_ref[p].astype(F32)
            rims_ref[pl.ds(to + RADIUS, inner), :] = clipped(main)
            for start in (0, cells_y - RADIUS):
                value = grid_ref[pl.ds(at + start, RADIUS), :]
                rims_ref[pl.ds(to + start, RADIUS), :] = clipped(value)

    @pl.loop(0, cells_y // chunk)
    def _(j):
        planes = []
        start = pl.multiple_of(j * chunk, chunk)
        for e in range(total):
            if RADIUS <= e < RADIUS + cells_x:
                at = pl.multiple_of(e * cells_y + start, chunk)
                value = clipped(grid_ref[pl.ds(at, chunk), :] - 0.5)
            else:
                side = e if e < RADIUS else e - cells_x
                value = rims_ref[pl.ds(pl.multiple_of(side * cells_y + start, chunk), chunk), :]
            planes.append(value)
        for i, value in enumerate(running(planes, cells_x)):
            smooth_ref[i, pl.ds(start, chunk), :] = value.astype(BF16)

    across = cone(iota((cells_y, cells_y), 0) - iota((cells_y, cells_y), 1))
    along = cone(iota((cells_z, cells_z), 0) - iota((cells_z, cells_z), 1))
    along = jnp.concatenate([along, along], axis=0)
    side = cone(iota((RADIUS, cells_z), 0) + zoff_ref[1] - iota((RADIUS, cells_z), 1))
    column = iota((cells_y, 2 * RADIUS), 1)
    place = jnp.where(column < RADIUS, column - RADIUS, column - RADIUS + cells_y)
    edge = cone(place - iota((cells_y, 2 * RADIUS), 0))
    z = iota((1, cells_z), 1) + zoff_ref[2]
    inside = jnp.zeros((1, cells_z), F32)
    for offset in range(-RADIUS, RADIUS + 1):
        good = (z + offset >= 0) & (z + offset < zoff_ref[3])
        inside = inside + jnp.where(good, float(TAPS - abs(offset)), 0.0)
    scale = 8.0 / (scale_total * inside)
    top = math.tanh(4.0)
    step = 4

    def copy(g):
        rows = pl.ds(pl.multiple_of(g * step * cells_y, 8), step * cells_y)
        return pltpu.make_async_copy(proj_ref.at[rows], out_ref.at[rows], sem.at[g])

    @pl.loop(0, cells_x // step)
    def _(g):
        rims = rim_ref[pl.ds(g * step, step)].reshape(step * RADIUS, cells_y)
        rims = dot(rims, across).astype(BF16)
        for pair in range(step // 2):
            x = g * step + 2 * pair
            both = jnp.concatenate([smooth_ref[x], smooth_ref[x + 1]], axis=1)
            both = dot(across, both)
            for k in range(2):
                half = jnp.concatenate(halves(both[:, k * cells_z : (k + 1) * cells_z]), axis=1)
                value = dot(half, along)
                at = (2 * pair + k) * RADIUS
                value = value + dot(rims[at : at + RADIUS], side, TN)
                ends = jnp.concatenate(
                    [before_ref[x + k].astype(F32), after_ref[x + k].astype(F32)], axis=0
                ).astype(BF16)
                value = value + dot(edge, ends)
                value = (top + jnp.tanh(value * scale)) * (1.0 / (2.0 * top))
                proj_ref[pl.ds(pl.multiple_of((x + k) * cells_y, 8), cells_y), :] = value
        copy(g).start()

    @pl.loop(0, partners)
    def _(p):
        for s in range(capacity):
            row = rows_ref[p * capacity + s]
            picked_ref[pl.ds(p * capacity + s, 1), :] = proj_ref[pl.ds(row, 1), :]

    ones = jnp.ones((8, cells_z), BF16)
    group = LANES // capacity

    @pl.loop(0, partners * capacity // LANES)
    def _(c):
        w = pay_ref[pl.ds(c * group, group), :capacity, :].reshape(LANES, cells_z)
        picked = picked_ref[pl.ds(pl.multiple_of(c * LANES, LANES), LANES), :]
        high, low = halves(w.astype(F32) * picked)
        amount = dot(ones, high, NT) + dot(ones, low, NT)
        ratio_ref[pl.ds(c, 1), :] = (amount / dot(ones, w, NT))[:1]

    @pl.loop(0, cells_x // step)
    def _(g):
        copy(g).wait()


def back_kernel(counts_ref, elements_ref, ratio_ref, out_ref):
    tiles, capacity = elements_ref.shape
    high_count = out_ref.shape[0]
    total = jnp.zeros(out_ref.shape, F32)
    for t in range(tiles):
        element = elements_ref[pl.ds(t, 1), :]
        live = iota((1, capacity), 1) < counts_ref[0, t]
        ratio = jnp.where(live, ratio_ref[pl.ds(t, 1), :], 0.0)
        lane = onehot(iota((LANES, capacity), 0) == (element & (LANES - 1)))
        spread = jnp.where(iota((high_count, capacity), 0) == element // LANES, ratio, 0.0)
        high, low = halves(spread)
        total = total + (dot(high, lane, NT) + dot(low, lane, NT))
    out_ref[...] = total


def body(
    design,
    forward_edges,
    adjoint_edges,
    edge_basis,
    quad_weights,
    slot_weights,
    slot_elements,
    slot_blocks,
    slot_counts,
):
    cells_x, cells_y, cells_z = design.shape
    tiles, capacity = slot_elements.shape
    n_tx, n_ty, n_gz = (lax.axis_size(a) for a in ("tx", "ty", "gz"))
    if cells_z != LANES or cells_y != 256 or n_gz != 2:
        raise NotImplementedError
    slots = 3 * capacity
    rows_ext = (cells_x + 2 * RADIUS) * cells_y
    gz = lax.axis_index("gz")
    zoff = jnp.stack(
        [
            jnp.where(gz == 0, cells_z - RADIUS, 0),
            jnp.where(gz == 0, cells_z, -RADIUS),
            gz * cells_z,
            jnp.int32(n_gz * cells_z),
        ]
    ).astype(jnp.int32)
    whole = pl.BlockSpec(memory_space=VMEM)
    scalars = pl.BlockSpec(memory_space=SMEM)
    anywhere = pl.BlockSpec(memory_space=pl.ANY)
    shape = jax.ShapeDtypeStruct
    params = lambda mib: pltpu.CompilerParams(vmem_limit_bytes=mib << 20)

    inner = cells_y - 2 * RADIUS
    edge_rows = 2 * RADIUS + RADIUS * cells_y // LANES
    payload, up_edge, down_edge, up_main, down_main = pl.pallas_call(
        functools.partial(pack_kernel, n_ty),
        out_shape=(
            shape((tiles, slots + 8, LANES), BF16),
            shape((RADIUS, edge_rows, LANES), BF16),
            shape((RADIUS, edge_rows, LANES), BF16),
            shape((RADIUS, inner, LANES), BF16),
            shape((RADIUS, inner, LANES), BF16),
        ),
        in_specs=[scalars] * 3 + [whole] * 6 + [anywhere],
        out_specs=(whole,) * 5,
        scratch_shapes=[
            VMEM((2 * RADIUS, cells_y, cells_z), F32),
            VMEM((4, tiles, LANES), F32),
            pltpu.SemaphoreType.DMA((2,)),
        ],
        compiler_params=params(16),
        name="pack",
    )(
        slot_counts,
        quad_weights,
        zoff,
        edge_basis.T,
        forward_edges.transpose(1, 0, 2),
        adjoint_edges.transpose(1, 0, 2),
        slot_weights,
        slot_elements,
        slot_blocks,
        design,
    )

    arrived = lax.all_to_all(payload, ("tx", "ty"), split_axis=0, concat_axis=0, tiled=True)
    up = [(i, (i + 1) % n_tx) for i in range(n_tx)]
    down = [(t, s) for s, t in up]
    low_edge = lax.ppermute(up_edge, "tx", up)
    high_edge = lax.ppermute(down_edge, "tx", down)
    low_main = lax.ppermute(up_main, "tx", up)
    high_main = lax.ppermute(down_main, "tx", down)

    meta = arrived[:, slots : slots + 3, :slots].astype(F32)
    rows = (meta[:, 0] * float(cells_y) + meta[:, 1]).astype(jnp.int32)
    vals = meta[:, 2]
    used = (rows >= 0) & (rows < rows_ext) & (vals != 0.0)
    rows_used = jnp.where(used, rows, -1).reshape(-1)
    rows_own = (rows[:, :capacity] - RADIUS * cells_y).reshape(-1)

    grid, edge_smooth, rim = pl.pallas_call(
        functools.partial(deposit_kernel, cells_y, slots),
        out_shape=(
            shape((rows_ext, cells_z), F32),
            shape((cells_x, 2 * RADIUS, cells_z), F32),
            shape((cells_x, RADIUS, cells_y), BF16),
        ),
        in_specs=[scalars] * 3 + [anywhere] + [whole] * 3,
        out_specs=(whole, whole, whole),
        scratch_shapes=[
            VMEM((cells_x + 2 * RADIUS, RADIUS, cells_y), F32),
            pltpu.SemaphoreType.DMA,
        ],
        compiler_params=params(16),
        name="deposit",
    )(
        rows_used, vals.reshape(-1), zoff, design.reshape(cells_x * cells_y, cells_z),
        low_edge, high_edge, arrived,
    )

    rim = lax.ppermute(rim, "gz", [(0, 1), (1, 0)])
    edge = shape((cells_x, RADIUS, cells_z), BF16)
    first, last = pl.pallas_call(
        edge_kernel,
        out_shape=(edge, edge),
        in_specs=[scalars, whole, whole],
        out_specs=(whole, whole),
        compiler_params=params(16),
        name="edges",
    )(zoff, edge_smooth, rim)
    up = [(i, (i + 1) % n_ty) for i in range(n_ty)]
    down = [(t, s) for s, t in up]
    before = lax.ppermute(last, "ty", up)
    after = lax.ppermute(first, "ty", down)

    projected, ratios = pl.pallas_call(
        functools.partial(finish_kernel, float(TAPS**4)),
        out_shape=(
            shape((cells_x * cells_y, cells_z), F32),
            shape((tiles * capacity // LANES, LANES), F32),
        ),
        in_specs=[scalars] * 2 + [whole] * 7,
        out_specs=(anywhere, whole),
        scratch_shapes=[
            VMEM((2 * RADIUS * cells_y, cells_z), F32),
            VMEM((cells_x, cells_y, cells_z), BF16),
            VMEM((cells_x * cells_y, cells_z), F32),
            VMEM((tiles * capacity, cells_z), F32),
            pltpu.SemaphoreType.DMA((cells_x // 4,)),
        ],
        compiler_params=params(24),
        name="finish",
    )(rows_own, zoff, grid, low_main, high_main, rim, before, after, arrived)

    ratios = ratios.reshape(tiles, capacity)
    ratios = lax.all_to_all(ratios, ("tx", "ty"), split_axis=0, concat_axis=0, tiled=True)
    elements = forward_edges.shape[2]
    density = pl.pallas_call(
        back_kernel,
        out_shape=shape((elements // LANES, LANES), F32),
        in_specs=[scalars, whole, whole],
        out_specs=whole,
        compiler_params=params(16),
        name="to_elements",
    )(slot_counts, slot_elements, ratios)
    return projected.reshape(design.shape), density.reshape(elements)


def solution(mesh):
    in_specs = (
        P("tx", "ty", "gz"),
        P(None, None, ("tx", "ty", "gz")),
        P(None, None, ("tx", "ty", "gz")),
        P(),
        P(),
        P(("tx", "ty", "gz"), None, None),
        P(("tx", "ty", "gz"), None),
        P(("tx", "ty", "gz"), None),
        P(("tx", "ty", "gz"), None),
    )
    out_specs = (P("tx", "ty", "gz"), P(("tx", "ty", "gz")))
    return jax.shard_map(body, mesh=mesh, in_specs=in_specs, out_specs=out_specs, check_vma=False)
```

```python
import functools
import math

import jax
import jax.numpy as jnp
from jax import lax
from jax.experimental import pallas as pl
from jax.experimental.pallas import tpu as pltpu
from jax.sharding import PartitionSpec as P


RADIUS = 8
LANES = 128
TAPS = RADIUS + 1
F32 = jnp.float32
BF16 = jnp.bfloat16
SMEM = pltpu.SMEM
VMEM = pltpu.VMEM
NT = ((1,), (1,))
TN = ((0,), (0,))


def iota(shape, dim):
    return lax.broadcasted_iota(jnp.int32, shape, dim)


def onehot(mask):
    return mask.astype(F32).astype(BF16)


def cone(distance):
    return jnp.maximum(TAPS - jnp.abs(distance), 0).astype(F32).astype(BF16)


def halves(x):
    high = x.astype(BF16)
    return high, (x - high.astype(F32)).astype(BF16)


def dot(a, b, contract=((1,), (0,)), precision=None):
    return lax.dot_general(
        a, b, (contract, ((), ())), preferred_element_type=F32, precision=precision
    )


def picker(first):
    return onehot(iota((RADIUS, LANES), 1) == iota((RADIUS, LANES), 0) + first)


def running(planes, length):
    add = lambda a, b: a + b
    box = [functools.reduce(add, planes[:TAPS])]
    for k in range(length + RADIUS - 1):
        box.append(box[-1] + (planes[k + TAPS] - planes[k]))
    total = functools.reduce(add, box[:TAPS])
    out = [total]
    for i in range(length - 1):
        total = total + (box[i + TAPS] - box[i])
        out.append(total)
    return out


def clipped(x):
    return jnp.clip(x, -0.5, 0.5)


def pack_kernel(
    n_ty, counts_ref, quad_ref, zoff_ref, basis_hbm, forward_hbm, adjoint_hbm, weights_hbm,
    elements_hbm, blocks_hbm, design_ref, pay_ref, up_edge_ref, down_edge_ref, basis_ref,
    forward_ref, adjoint_ref, weights_ref, elements_ref, blocks_ref, strip_ref, code_ref, sem,
):
    sources = (forward_hbm, adjoint_hbm, basis_hbm, elements_hbm, blocks_hbm, weights_hbm)
    targets = (forward_ref, adjoint_ref, basis_ref, elements_ref, blocks_ref, weights_ref)
    loads = [
        pltpu.make_async_copy(source, target, sem.at[2 + i])
        for i, (source, target) in enumerate(zip(sources, targets))
    ]
    for load in loads:
        load.start()
    cells_x, cells_y, _ = design_ref.shape
    tiles, capacity = elements_ref.shape
    points = quad_ref.shape[0]
    highest = lax.Precision.HIGHEST
    copies = [
        pltpu.make_async_copy(
            design_ref.at[pl.ds(start, RADIUS)], strip_ref.at[pl.ds(side * RADIUS, RADIUS)],
            sem.at[side],
        )
        for side, start in enumerate((0, cells_x - RADIUS))
    ]
    for copy in copies:
        copy.start()
    for load in loads:
        load.wait()

    terms, edges = 2 * forward_ref.shape[0], forward_ref.shape[0]
    point = iota((1, 3 * points), 1) % points
    quad = jnp.zeros((1, 3 * points), F32)
    for q in range(points):
        quad = quad + jnp.where(point == q, quad_ref[q], 0.0)
    twice = (iota((terms, edges), 0) // 2 == iota((terms, edges), 1)).astype(F32)
    basis = dot(twice, basis_ref[...], precision=highest)
    gram = dot(basis * quad, basis, NT, precision=highest)
    row, column = iota((terms, terms), 0), iota((terms, terms), 1)
    gram = jnp.where(row % 2 == 0, gram, -gram)
    gram = jnp.where(row % 2 == column % 2, gram, 0.0)
    adjoint = jnp.concatenate([adjoint_ref[k] for k in range(edges)], axis=0)
    forward = jnp.concatenate([forward_ref[k] for k in range(edges)], axis=0)
    sens = jnp.sum(forward * dot(gram, adjoint, precision=highest), axis=0, keepdims=True)
    groups = sens.shape[1] // LANES
    sens = jnp.concatenate([sens[:, g * LANES : (g + 1) * LANES] for g in range(groups)], axis=0)
    first, _ = halves(sens)
    second, third = halves(sens - first.astype(F32))
    parts = jnp.concatenate([first, second, third], axis=0)

    element, block = elements_ref[...], blocks_ref[...]
    codes = [
        element // LANES,
        element % LANES,
        block // cells_y + RADIUS,
        block % cells_y,
    ]
    place = iota((capacity, LANES), 1) - iota((capacity, LANES), 0)
    for index, code in enumerate(codes):
        code = code.astype(F32).astype(BF16)
        total = jnp.zeros((tiles, LANES), F32)
        for order, d in enumerate((0, -1, 1)):
            moved = dot(code, onehot(place == order * capacity))
            shift = (d * n_ty) % tiles
            if shift:
                moved = jnp.concatenate([moved[shift:], moved[:shift]], axis=0)
            if index == 2 and d:
                group = iota((tiles, LANES), 1) // capacity
                moved = moved + jnp.where(group == order, float(d * cells_x), 0.0)
            total = total + moved
        code_ref[index] = total

    @pl.loop(0, tiles, unroll=min(tiles, 16))
    def _(t):
        high, low, plane, line = (code_ref[index, pl.ds(t, 1), :] for index in range(4))
        lane = iota((1, LANES), 1)
        live = jnp.zeros((1, LANES), jnp.bool_)
        sources = []
        for order, d in enumerate((0, -1, 1)):
            source = lax.rem(t + (d * n_ty) % tiles, tiles)
            sources.append(source)
            at = lane - order * capacity
            live = live | ((at >= 0) & (at < capacity) & (at < counts_ref[0, source]))
        hit = onehot(iota((LANES, LANES), 0).astype(F32) == low)
        found = dot(parts, hit)
        found = (found[:groups] + found[groups : 2 * groups]) + found[2 * groups :]
        mine = iota((groups, LANES), 0).astype(F32) == high
        value = jnp.sum(jnp.where(mine, found, 0.0), axis=0, keepdims=True)
        value = jnp.where(live, value, 0.0).astype(BF16).astype(F32) * -0.5
        kind = iota((8, LANES), 0)
        meta = jnp.where(kind == 0, plane, jnp.where(kind == 1, line, value))
        meta = jnp.where(kind < 3, meta, 0.0)
        for order, source in enumerate(sources):
            pay_ref[t, order * capacity : (order + 1) * capacity, :] = weights_ref[source]
        pay_ref[t, 3 * capacity :, :] = meta.astype(BF16)

    pick = picker(zoff_ref[0])
    for side, edge_ref in enumerate((down_edge_ref, up_edge_ref)):
        copies[side].wait()

        @pl.loop(0, RADIUS, unroll=4)
        def _(p):
            plane = strip_ref[side * RADIUS + p] - 0.5
            edge_ref[p, :RADIUS] = plane[:RADIUS].astype(BF16)
            edge_ref[p, RADIUS : 2 * RADIUS] = plane[cells_y - RADIUS :].astype(BF16)
            flipped = dot(pick, plane.astype(BF16), NT).astype(BF16)
            for k in range(cells_y // LANES):
                start = (2 + k) * RADIUS
                edge_ref[p, start : start + RADIUS] = flipped[:, k * LANES : (k + 1) * LANES]


def main_kernel(design_ref, token_ref, up_ref, down_ref, strip_ref, sem):
    cells_x, cells_y, _ = design_ref.shape
    copies = [
        pltpu.make_async_copy(
            design_ref.at[pl.ds(start, RADIUS)], strip_ref.at[pl.ds(side * RADIUS, RADIUS)],
            sem.at[side],
        )
        for side, start in enumerate((0, cells_x - RADIUS))
    ]
    for copy in copies:
        copy.start()
    for side, main_ref in enumerate((down_ref, up_ref)):
        copies[side].wait()

        @pl.loop(0, RADIUS, unroll=2)
        def _(p):
            plane = strip_ref[side * RADIUS + p, RADIUS : cells_y - RADIUS, :]
            main_ref[p] = (plane - 0.5).astype(BF16)


def deposit_kernel(
    cells_y, slots, zoff_ref, design_ref, low_ref, high_ref, pay_ref, grid_ref, rows_out_ref,
    rim_ref, own_ref, flip_ref, weight_ref, code_ref, value_ref, code_smem, value_smem, sem,
):
    cells_x = design_ref.shape[0] // cells_y
    partners = pay_ref.shape[0]
    rim = RADIUS * cells_y
    own = cells_x * cells_y
    copy = pltpu.make_async_copy(design_ref, grid_ref.at[pl.ds(rim, own)], sem.at[0])
    copy.start()

    lane = iota((1, LANES), 1)
    upper = onehot(iota((LANES, LANES), 0) <= iota((LANES, LANES), 1))

    @pl.loop(0, partners, unroll=min(partners, 16))
    def _(p):
        weight_ref[pl.ds(pl.multiple_of(p * slots, 16), slots), :] = pay_ref[p, :slots, :].astype(F32)
        meta = pay_ref[p, slots : slots + 8, :].astype(F32)
        plane, line, value = meta[0:1], meta[1:2], meta[2:3]
        own_ref[pl.ds(p, 1), :] = ((plane - float(RADIUS)) * float(cells_y) + line).astype(jnp.int32)
        used = (plane >= 0.0) & (plane < float(cells_x + 2 * RADIUS)) & (value != 0.0)
        used = jnp.where(used & (lane < slots), 1.0, 0.0)
        order = dot(jnp.broadcast_to(used, (8, LANES)).astype(BF16), upper)[:1]
        place = jnp.where(used > 0.0, order - 1.0, -1.0)
        hit = onehot(iota((LANES, LANES), 0).astype(F32) == place)
        kind = iota((8, LANES), 0)
        meta = jnp.where(kind == 3, lane.astype(F32), jnp.where(kind < 3, meta, 0.0))
        moved = dot(meta.astype(BF16), hit, NT)
        code = (moved[0:1] * float(cells_y) + moved[1:2]) * float(LANES) + moved[3:4]
        code = jnp.where(lane == LANES - 1, order[:, LANES - 1 :], code)
        code_ref[pl.ds(p, 1), :] = code.astype(jnp.int32)
        value_ref[pl.ds(p, 1), :] = moved[2:3]

    lists = [
        pltpu.make_async_copy(code_ref, code_smem, sem.at[1]),
        pltpu.make_async_copy(value_ref, value_smem, sem.at[2]),
    ]
    for move in lists:
        move.start()
    zeros = jnp.zeros((cells_y, LANES), F32)
    for p in range(RADIUS):
        grid_ref[p * cells_y : (p + 1) * cells_y, :] = zeros
        grid_ref[rim + own + p * cells_y : rim + own + (p + 1) * cells_y, :] = zeros
    for move in lists:
        move.wait()
    copy.wait()

    @pl.loop(0, partners)
    def _(p):
        @pl.loop(0, (code_smem[p, LANES - 1] + 3) // 4)
        def _(j):
            for k in range(4):
                code = code_smem[p, j * 4 + k]
                row = code // LANES
                amount = value_smem[p, j * 4 + k] * weight_ref[pl.ds(p * slots + code % LANES, 1), :]
                grid_ref[pl.ds(row, 1), :] = grid_ref[pl.ds(row, 1), :] + amount

    total = cells_x + 2 * RADIUS
    pick = picker(zoff_ref[0])

    @pl.loop(0, cells_x, unroll=4)
    def _(x):
        plane = clipped(grid_ref[pl.ds(rim + x * cells_y, cells_y), :] - 0.5)
        flip_ref[x + RADIUS] = dot(pick, plane.astype(BF16), NT)

    for source_ref, base in ((low_ref, 0), (high_ref, RADIUS + cells_x)):
        @pl.loop(0, RADIUS, unroll=4)
        def _(p):
            plane = grid_ref[pl.ds((base + p) * cells_y, cells_y), :]
            deposited = dot(pick, plane.astype(BF16), NT)
            raw = jnp.concatenate(
                [
                    source_ref[p, (2 + k) * RADIUS : (3 + k) * RADIUS].astype(F32)
                    for k in range(cells_y // LANES)
                ],
                axis=1,
            )
            flip_ref[base + p] = clipped(raw + deposited)

    for source_ref, base in ((low_ref, 0), (high_ref, RADIUS + cells_x)):
        for p in range(RADIUS):
            for k, start in enumerate((0, cells_y - RADIUS)):
                at = (base + p) * cells_y + start
                edge = source_ref[p, k * RADIUS : (k + 1) * RADIUS].astype(F32)
                grid_ref[at : at + RADIUS, :] = grid_ref[at : at + RADIUS, :] + edge

    for k, start in enumerate((0, cells_y - RADIUS)):
        planes = []
        for e in range(total):
            at = e * cells_y + start
            bias = 0.5 if RADIUS <= e < RADIUS + cells_x else 0.0
            planes.append(clipped(grid_ref[at : at + RADIUS, :] - bias))
        for i, value in enumerate(running(planes, cells_x)):
            rows_out_ref[i, k * RADIUS : (k + 1) * RADIUS, :] = value

    for i, value in enumerate(running([flip_ref[e] for e in range(total)], cells_x)):
        rim_ref[i] = value.astype(BF16)


def edge_kernel(zoff_ref, rows_ref, rim_ref, first_ref, last_ref):
    cells_x, double, cells_z = rows_ref.shape
    cells_y = rim_ref.shape[2]
    weights = cone(iota((cells_z, cells_z), 0) - iota((cells_z, cells_z), 1))
    weights = jnp.concatenate([weights, weights], axis=0)
    side = cone(iota((RADIUS, cells_z), 0) + zoff_ref[1] - iota((RADIUS, cells_z), 1))
    rows = rows_ref[...].reshape(cells_x * double, cells_z)
    value = dot(jnp.concatenate(halves(rows), axis=1), weights)
    for x in range(cells_x):
        for k, out_ref in enumerate((first_ref, last_ref)):
            start = 0 if k == 0 else cells_y - LANES
            shift = 0 if k == 0 else LANES - RADIUS
            rim = rim_ref[x, :, start : start + LANES][:, shift : shift + RADIUS]
            at = x * double + k * RADIUS
            out_ref[x] = (value[at : at + RADIUS] + dot(rim, side, TN)).astype(BF16)


def finish_kernel(
    scale_total, zoff_ref, own_ref, grid_ref, low_ref, high_ref, rim_ref, before_ref, after_ref,
    pay_ref, out_ref, ratio_ref, rims_ref, smooth_ref, proj_ref, picked_ref, rows_ref, sem, own_sem,
):
    cells_x, _, cells_y = rim_ref.shape
    cells_z = out_ref.shape[1]
    partners = pay_ref.shape[0]
    capacity = picked_ref.shape[0] // partners
    total = cells_x + 2 * RADIUS
    inner = cells_y - 2 * RADIUS
    chunk = 16
    fetch = pltpu.make_async_copy(own_ref, rows_ref, own_sem)
    fetch.start()

    for source_ref, base, into in ((low_ref, 0, 0), (high_ref, RADIUS + cells_x, RADIUS)):
        @pl.loop(0, RADIUS)
        def _(p):
            at = pl.multiple_of((base + p) * cells_y, 8)
            to = pl.multiple_of((into + p) * cells_y, 8)
            main = grid_ref[pl.ds(at + RADIUS, inner), :] + source_ref[p].astype(F32)
            rims_ref[pl.ds(to + RADIUS, inner), :] = clipped(main)
            for start in (0, cells_y - RADIUS):
                value = grid_ref[pl.ds(at + start, RADIUS), :]
                rims_ref[pl.ds(to + start, RADIUS), :] = clipped(value)

    @pl.loop(0, cells_y // chunk)
    def _(j):
        planes = []
        start = pl.multiple_of(j * chunk, chunk)
        for e in range(total):
            if RADIUS <= e < RADIUS + cells_x:
                at = pl.multiple_of(e * cells_y + start, chunk)
                value = clipped(grid_ref[pl.ds(at, chunk), :] - 0.5)
            else:
                side = e if e < RADIUS else e - cells_x
                value = rims_ref[pl.ds(pl.multiple_of(side * cells_y + start, chunk), chunk), :]
            planes.append(value)
        for i, value in enumerate(running(planes, cells_x)):
            smooth_ref[i, pl.ds(start, chunk), :] = value.astype(BF16)

    across = cone(iota((cells_y, cells_y), 0) - iota((cells_y, cells_y), 1))
    along = cone(iota((cells_z, cells_z), 0) - iota((cells_z, cells_z), 1))
    along = jnp.concatenate([along, along], axis=0)
    side = cone(iota((RADIUS, cells_z), 0) + zoff_ref[1] - iota((RADIUS, cells_z), 1))
    column = iota((cells_y, 2 * RADIUS), 1)
    place = jnp.where(column < RADIUS, column - RADIUS, column - RADIUS + cells_y)
    edge = cone(place - iota((cells_y, 2 * RADIUS), 0))
    z = iota((1, cells_z), 1) + zoff_ref[2]
    inside = jnp.zeros((1, cells_z), F32)
    for offset in range(-RADIUS, RADIUS + 1):
        good = (z + offset >= 0) & (z + offset < zoff_ref[3])
        inside = inside + jnp.where(good, float(TAPS - abs(offset)), 0.0)
    scale = 8.0 / (scale_total * inside)
    top = math.tanh(4.0)
    step = 4

    def copy(g):
        rows = pl.ds(pl.multiple_of(g * step * cells_y, 8), step * cells_y)
        return pltpu.make_async_copy(proj_ref.at[rows], out_ref.at[rows], sem.at[g])

    @pl.loop(0, cells_x // step)
    def _(g):
        rims = rim_ref[pl.ds(g * step, step)].reshape(step * RADIUS, cells_y)
        rims = dot(rims, across).astype(BF16)
        for pair in range(step // 2):
            x = g * step + 2 * pair
            both = jnp.concatenate([smooth_ref[x], smooth_ref[x + 1]], axis=1)
            both = dot(across, both)
            for k in range(2):
                half = jnp.concatenate(halves(both[:, k * cells_z : (k + 1) * cells_z]), axis=1)
                value = dot(half, along)
                at = (2 * pair + k) * RADIUS
                value = value + dot(rims[at : at + RADIUS], side, TN)
                ends = jnp.concatenate(
                    [before_ref[x + k].astype(F32), after_ref[x + k].astype(F32)], axis=0
                ).astype(BF16)
                value = value + dot(edge, ends)
                value = (top + jnp.tanh(value * scale)) * (1.0 / (2.0 * top))
                proj_ref[pl.ds(pl.multiple_of((x + k) * cells_y, 8), cells_y), :] = value
        copy(g).start()

    fetch.wait()

    @pl.loop(0, partners)
    def _(p):
        for s in range(capacity):
            row = rows_ref[p, s]
            picked_ref[pl.ds(p * capacity + s, 1), :] = proj_ref[pl.ds(row, 1), :]

    ones = jnp.ones((8, cells_z), BF16)
    group = LANES // capacity

    @pl.loop(0, partners * capacity // LANES)
    def _(c):
        w = pay_ref[pl.ds(c * group, group), :capacity, :].reshape(LANES, cells_z)
        picked = picked_ref[pl.ds(pl.multiple_of(c * LANES, LANES), LANES), :]
        high, low = halves(w.astype(F32) * picked)
        amount = dot(ones, high, NT) + dot(ones, low, NT)
        ratio_ref[pl.ds(c, 1), :] = (amount / dot(ones, w, NT))[:1]

    @pl.loop(0, cells_x // step)
    def _(g):
        copy(g).wait()


def back_kernel(counts_ref, elements_ref, ratio_ref, out_ref):
    tiles, capacity = elements_ref.shape
    high_count = out_ref.shape[0]
    total = jnp.zeros(out_ref.shape, F32)
    for t in range(tiles):
        element = elements_ref[pl.ds(t, 1), :]
        live = iota((1, capacity), 1) < counts_ref[0, t]
        ratio = jnp.where(live, ratio_ref[pl.ds(t, 1), :], 0.0)
        lane = onehot(iota((LANES, capacity), 0) == (element & (LANES - 1)))
        spread = jnp.where(iota((high_count, capacity), 0) == element // LANES, ratio, 0.0)
        high, low = halves(spread)
        total = total + (dot(high, lane, NT) + dot(low, lane, NT))
    out_ref[...] = total


def update(
    design,
    forward_edges,
    adjoint_edges,
    edge_basis,
    quad_weights,
    slot_weights,
    slot_elements,
    slot_blocks,
    slot_counts,
):
    cells_x, cells_y, cells_z = design.shape
    tiles, capacity = slot_elements.shape
    n_tx, n_ty, n_gz = (lax.axis_size(a) for a in ("tx", "ty", "gz"))
    if cells_z != LANES or cells_y != 256 or n_gz != 2:
        raise NotImplementedError
    slots = 3 * capacity
    edge_count, elements = forward_edges.shape[1:]
    rows_ext = (cells_x + 2 * RADIUS) * cells_y
    gz = lax.axis_index("gz")
    zoff = jnp.stack(
        [
            jnp.where(gz == 0, cells_z - RADIUS, 0),
            jnp.where(gz == 0, cells_z, -RADIUS),
            gz * cells_z,
            jnp.int32(n_gz * cells_z),
        ]
    ).astype(jnp.int32)
    whole = pl.BlockSpec(memory_space=VMEM)
    scalars = pl.BlockSpec(memory_space=SMEM)
    anywhere = pl.BlockSpec(memory_space=pltpu.HBM)
    shape = jax.ShapeDtypeStruct
    params = lambda mib: pltpu.CompilerParams(vmem_limit_bytes=mib << 20)

    inner = cells_y - 2 * RADIUS
    edge_rows = 2 * RADIUS + RADIUS * cells_y // LANES
    payload, up_edge, down_edge = pl.pallas_call(
        functools.partial(pack_kernel, n_ty),
        out_shape=(
            shape((tiles, slots + 8, LANES), BF16),
            shape((RADIUS, edge_rows, LANES), BF16),
            shape((RADIUS, edge_rows, LANES), BF16),
        ),
        in_specs=[scalars] * 3 + [anywhere] * 7,
        out_specs=(whole,) * 3,
        scratch_shapes=[
            VMEM(edge_basis.shape[::-1], F32),
            VMEM((edge_count, 2, elements), F32),
            VMEM((edge_count, 2, elements), F32),
            VMEM(slot_weights.shape, BF16),
            VMEM(slot_elements.shape, jnp.int32),
            VMEM(slot_blocks.shape, jnp.int32),
            VMEM((2 * RADIUS, cells_y, cells_z), F32),
            VMEM((4, tiles, LANES), F32),
            pltpu.SemaphoreType.DMA((8,)),
        ],
        name="pack",
    )(
        slot_counts,
        quad_weights,
        zoff,
        edge_basis.T,
        forward_edges.transpose(1, 0, 2),
        adjoint_edges.transpose(1, 0, 2),
        slot_weights,
        slot_elements,
        slot_blocks,
        design,
    )

    arrived = lax.all_to_all(payload, ("tx", "ty"), split_axis=0, concat_axis=0, tiled=True)
    up = [(i, (i + 1) % n_tx) for i in range(n_tx)]
    down = [(t, s) for s, t in up]
    low_edge = lax.ppermute(up_edge, "tx", up)
    high_edge = lax.ppermute(down_edge, "tx", down)
    main = shape((RADIUS, inner, LANES), BF16)
    call = pl.pallas_call(
        main_kernel,
        out_shape=(main, main),
        in_specs=[anywhere, anywhere],
        out_specs=(whole, whole),
        scratch_shapes=[
            VMEM((2 * RADIUS, cells_y, cells_z), F32),
            pltpu.SemaphoreType.DMA((2,)),
        ],
        name="main_rims",
    )
    up_main, down_main = call(design, up_edge)
    low_main = lax.ppermute(up_main, "tx", up)
    high_main = lax.ppermute(down_main, "tx", down)

    grid, edge_smooth, rim, rows_own = pl.pallas_call(
        functools.partial(deposit_kernel, cells_y, slots),
        out_shape=(
            shape((rows_ext, cells_z), F32),
            shape((cells_x, 2 * RADIUS, cells_z), F32),
            shape((cells_x, RADIUS, cells_y), BF16),
            shape((tiles, LANES), jnp.int32),
        ),
        in_specs=[scalars, anywhere] + [whole] * 3,
        out_specs=(whole,) * 4,
        scratch_shapes=[
            VMEM((cells_x + 2 * RADIUS, RADIUS, cells_y), F32),
            VMEM((tiles * slots, LANES), F32),
            VMEM((tiles, LANES), jnp.int32),
            VMEM((tiles, LANES), F32),
            SMEM((tiles, LANES), jnp.int32),
            SMEM((tiles, LANES), F32),
            pltpu.SemaphoreType.DMA((3,)),
        ],
        compiler_params=params(16),
        name="deposit",
    )(zoff, design.reshape(cells_x * cells_y, cells_z), low_edge, high_edge, arrived)

    rim = lax.ppermute(rim, "gz", [(0, 1), (1, 0)])
    edge = shape((cells_x, RADIUS, cells_z), BF16)
    first, last = pl.pallas_call(
        edge_kernel,
        out_shape=(edge, edge),
        in_specs=[scalars, whole, whole],
        out_specs=(whole, whole),
        compiler_params=params(16),
        name="edges",
    )(zoff, edge_smooth, rim)
    up = [(i, (i + 1) % n_ty) for i in range(n_ty)]
    down = [(t, s) for s, t in up]
    before = lax.ppermute(last, "ty", up)
    after = lax.ppermute(first, "ty", down)

    projected, ratios = pl.pallas_call(
        functools.partial(finish_kernel, float(TAPS**4)),
        out_shape=(
            shape((cells_x * cells_y, cells_z), F32),
            shape((tiles * capacity // LANES, LANES), F32),
        ),
        in_specs=[scalars] + [whole] * 8,
        out_specs=(anywhere, whole),
        scratch_shapes=[
            VMEM((2 * RADIUS * cells_y, cells_z), F32),
            VMEM((cells_x, cells_y, cells_z), BF16),
            VMEM((cells_x * cells_y, cells_z), F32),
            VMEM((tiles * capacity, cells_z), F32),
            SMEM((tiles, LANES), jnp.int32),
            pltpu.SemaphoreType.DMA((cells_x // 4,)),
            pltpu.SemaphoreType.DMA,
        ],
        compiler_params=params(24),
        name="finish",
    )(zoff, rows_own, grid, low_main, high_main, rim, before, after, arrived)

    ratios = ratios.reshape(tiles, capacity)
    ratios = lax.all_to_all(ratios, ("tx", "ty"), split_axis=0, concat_axis=0, tiled=True)
    density = pl.pallas_call(
        back_kernel,
        out_shape=shape((elements // LANES, LANES), F32),
        in_specs=[scalars, whole, whole],
        out_specs=whole,
        compiler_params=params(16),
        name="to_elements",
    )(slot_counts, slot_elements, ratios)
    return projected.reshape(design.shape), density.reshape(elements)


def solution(mesh):
    in_specs = (
        P("tx", "ty", "gz"),
        P(None, None, ("tx", "ty", "gz")),
        P(None, None, ("tx", "ty", "gz")),
        P(),
        P(),
        P(("tx", "ty", "gz"), None, None),
        P(("tx", "ty", "gz"), None),
        P(("tx", "ty", "gz"), None),
        P(("tx", "ty", "gz"), None),
    )
    out_specs = (P("tx", "ty", "gz"), P(("tx", "ty", "gz")))
    return jax.shard_map(update, mesh=mesh, in_specs=in_specs, out_specs=out_specs, check_vma=False)
```

```python
import functools
import math

import jax
import jax.numpy as jnp
from jax import lax
from jax.experimental import pallas as pl
from jax.experimental.pallas import tpu as pltpu
from jax.sharding import PartitionSpec as P


RADIUS = 8
LANES = 128
TAPS = RADIUS + 1
F32 = jnp.float32
BF16 = jnp.bfloat16
SMEM = pltpu.SMEM
VMEM = pltpu.VMEM
NT = ((1,), (1,))
TN = ((0,), (0,))


def iota(shape, dim):
    return lax.broadcasted_iota(jnp.int32, shape, dim)


def onehot(mask):
    return mask.astype(F32).astype(BF16)


def cone(distance):
    return jnp.maximum(TAPS - jnp.abs(distance), 0).astype(F32).astype(BF16)


def halves(x):
    high = x.astype(BF16)
    return high, (x - high.astype(F32)).astype(BF16)


def dot(a, b, contract=((1,), (0,)), precision=None):
    return lax.dot_general(
        a, b, (contract, ((), ())), preferred_element_type=F32, precision=precision
    )


def picker():
    first = jnp.where(lax.axis_index("gz") == 0, LANES - RADIUS, 0)
    return onehot(iota((RADIUS, LANES), 1) == iota((RADIUS, LANES), 0) + first)


def side_weights():
    first = jnp.where(lax.axis_index("gz") == 0, LANES, -RADIUS)
    return cone(iota((RADIUS, LANES), 0) + first - iota((RADIUS, LANES), 1))


def running(planes, length):
    add = lambda a, b: a + b
    box = [functools.reduce(add, planes[:TAPS])]
    for k in range(length + RADIUS - 1):
        box.append(box[-1] + (planes[k + TAPS] - planes[k]))
    total = functools.reduce(add, box[:TAPS])
    out = [total]
    for i in range(length - 1):
        total = total + (box[i + TAPS] - box[i])
        out.append(total)
    return out


def clipped(x):
    return jnp.clip(x, -0.5, 0.5)


def pack_kernel(
    n_ty, cells_x, cells_y, counts_hbm, quad_hbm, basis_hbm, forward_hbm, adjoint_hbm, weights_hbm,
    elements_hbm, blocks_hbm, pay_ref, basis_ref, forward_ref, adjoint_ref, weights_ref,
    elements_ref, blocks_ref, counts_ref, quad_ref, code_ref, sem,
):
    sources = (forward_hbm, adjoint_hbm, basis_hbm, elements_hbm, blocks_hbm, weights_hbm)
    sources += (counts_hbm, quad_hbm)
    targets = (forward_ref, adjoint_ref, basis_ref, elements_ref, blocks_ref, weights_ref)
    targets += (counts_ref, quad_ref)
    loads = [
        pltpu.make_async_copy(source, target, sem.at[i])
        for i, (source, target) in enumerate(zip(sources, targets))
    ]
    for load in loads:
        load.start()
    tiles, capacity = elements_ref.shape
    points = quad_ref.shape[0]
    highest = lax.Precision.HIGHEST
    for load in loads:
        load.wait()

    terms, edges = 2 * forward_ref.shape[0], forward_ref.shape[0]
    point = iota((1, 3 * points), 1) % points
    quad = jnp.zeros((1, 3 * points), F32)
    for q in range(points):
        quad = quad + jnp.where(point == q, quad_ref[q], 0.0)
    twice = (iota((terms, edges), 0) // 2 == iota((terms, edges), 1)).astype(F32)
    basis = dot(twice, basis_ref[...], precision=highest)
    gram = dot(basis * quad, basis, NT, precision=highest)
    row, column = iota((terms, terms), 0), iota((terms, terms), 1)
    gram = jnp.where(row % 2 == 0, gram, -gram)
    gram = jnp.where(row % 2 == column % 2, gram, 0.0)
    adjoint = jnp.concatenate([adjoint_ref[k] for k in range(edges)], axis=0)
    forward = jnp.concatenate([forward_ref[k] for k in range(edges)], axis=0)
    sens = jnp.sum(forward * dot(gram, adjoint, precision=highest), axis=0, keepdims=True)
    groups = sens.shape[1] // LANES
    sens = jnp.concatenate([sens[:, g * LANES : (g + 1) * LANES] for g in range(groups)], axis=0)
    first, _ = halves(sens)
    second, third = halves(sens - first.astype(F32))
    parts = jnp.concatenate([first, second, third], axis=0)

    element, block = elements_ref[...], blocks_ref[...]
    codes = [
        element // LANES,
        element % LANES,
        block // cells_y + RADIUS,
        block % cells_y,
    ]
    place = iota((capacity, LANES), 1) - iota((capacity, LANES), 0)
    for index, code in enumerate(codes):
        code = code.astype(F32).astype(BF16)
        total = jnp.zeros((tiles, LANES), F32)
        for order, d in enumerate((0, -1, 1)):
            moved = dot(code, onehot(place == order * capacity))
            shift = (d * n_ty) % tiles
            if shift:
                moved = jnp.concatenate([moved[shift:], moved[:shift]], axis=0)
            if index == 2 and d:
                group = iota((tiles, LANES), 1) // capacity
                moved = moved + jnp.where(group == order, float(d * cells_x), 0.0)
            total = total + moved
        code_ref[index] = total

    @pl.loop(0, tiles, unroll=min(tiles, 16))
    def _(t):
        high, low, plane, line = (code_ref[index, pl.ds(t, 1), :] for index in range(4))
        lane = iota((1, LANES), 1)
        live = jnp.zeros((1, LANES), jnp.bool_)
        sources = []
        for order, d in enumerate((0, -1, 1)):
            source = lax.rem(t + (d * n_ty) % tiles, tiles)
            sources.append(source)
            at = lane - order * capacity
            live = live | ((at >= 0) & (at < capacity) & (at < counts_ref[0, source]))
        hit = onehot(iota((LANES, LANES), 0).astype(F32) == low)
        found = dot(parts, hit)
        found = (found[:groups] + found[groups : 2 * groups]) + found[2 * groups :]
        mine = iota((groups, LANES), 0).astype(F32) == high
        value = jnp.sum(jnp.where(mine, found, 0.0), axis=0, keepdims=True)
        value = jnp.where(live, value, 0.0).astype(BF16).astype(F32) * -0.5
        kind = iota((8, LANES), 0)
        meta = jnp.where(kind == 0, plane, jnp.where(kind == 1, line, value))
        meta = jnp.where(kind < 3, meta, 0.0)
        for order, source in enumerate(sources):
            pay_ref[t, order * capacity : (order + 1) * capacity, :] = weights_ref[source]
        pay_ref[t, 3 * capacity :, :] = meta.astype(BF16)


def strips(design_ref, strip_ref, sem):
    cells_x = design_ref.shape[0]
    return [
        pltpu.make_async_copy(
            design_ref.at[pl.ds(start, RADIUS)], strip_ref.at[pl.ds(side * RADIUS, RADIUS)],
            sem.at[side],
        )
        for side, start in enumerate((0, cells_x - RADIUS))
    ]


def cast_edge_kernel(design_ref, token_ref, up_edge_ref, down_edge_ref, strip_ref, sem):
    cells_y = design_ref.shape[1]
    copies = strips(design_ref, strip_ref, sem)
    for copy in copies:
        copy.start()
    pick = picker()
    for side, edge_ref in enumerate((down_edge_ref, up_edge_ref)):
        copies[side].wait()

        @pl.loop(0, RADIUS, unroll=4)
        def _(p):
            plane = strip_ref[side * RADIUS + p] - 0.5
            edge_ref[p, :RADIUS] = plane[:RADIUS].astype(BF16)
            edge_ref[p, RADIUS : 2 * RADIUS] = plane[cells_y - RADIUS :].astype(BF16)
            flipped = dot(pick, plane.astype(BF16), NT).astype(BF16)
            for k in range(cells_y // LANES):
                start = (2 + k) * RADIUS
                edge_ref[p, start : start + RADIUS] = flipped[:, k * LANES : (k + 1) * LANES]


def cast_main_kernel(design_ref, token_ref, up_ref, down_ref, strip_ref, sem):
    cells_y = design_ref.shape[1]
    copies = strips(design_ref, strip_ref, sem)
    for copy in copies:
        copy.start()
    for side, main_ref in enumerate((down_ref, up_ref)):
        copies[side].wait()

        @pl.loop(0, RADIUS, unroll=2)
        def _(p):
            plane = strip_ref[side * RADIUS + p, RADIUS : cells_y - RADIUS, :]
            main_ref[p] = (plane - 0.5).astype(BF16)


def deposit_kernel(
    cells_y, slots, design_ref, low_ref, high_ref, pay_ref, grid_ref, rows_out_ref,
    rim_ref, own_ref, flip_ref, weight_ref, code_ref, value_ref, code_smem, value_smem, sem,
):
    cells_x = design_ref.shape[0] // cells_y
    partners = pay_ref.shape[0]
    rim = RADIUS * cells_y
    own = cells_x * cells_y
    copy = pltpu.make_async_copy(design_ref, grid_ref.at[pl.ds(rim, own)], sem.at[0])
    copy.start()

    lane = iota((1, LANES), 1)
    upper = onehot(iota((LANES, LANES), 0) <= iota((LANES, LANES), 1))

    @pl.loop(0, partners, unroll=min(partners, 16))
    def _(p):
        weight_ref[pl.ds(pl.multiple_of(p * slots, 16), slots), :] = pay_ref[p, :slots, :].astype(F32)
        meta = pay_ref[p, slots : slots + 8, :].astype(F32)
        plane, line, value = meta[0:1], meta[1:2], meta[2:3]
        own_ref[pl.ds(p, 1), :] = ((plane - float(RADIUS)) * float(cells_y) + line).astype(jnp.int32)
        used = (plane >= 0.0) & (plane < float(cells_x + 2 * RADIUS)) & (value != 0.0)
        used = jnp.where(used & (lane < slots), 1.0, 0.0)
        order = dot(jnp.broadcast_to(used, (8, LANES)).astype(BF16), upper)[:1]
        place = jnp.where(used > 0.0, order - 1.0, -1.0)
        hit = onehot(iota((LANES, LANES), 0).astype(F32) == place)
        kind = iota((8, LANES), 0)
        meta = jnp.where(kind == 3, lane.astype(F32), jnp.where(kind < 3, meta, 0.0))
        moved = dot(meta.astype(BF16), hit, NT)
        code = (moved[0:1] * float(cells_y) + moved[1:2]) * float(LANES) + moved[3:4]
        code = jnp.where(lane == LANES - 1, order[:, LANES - 1 :], code)
        code_ref[pl.ds(p, 1), :] = code.astype(jnp.int32)
        value_ref[pl.ds(p, 1), :] = moved[2:3]

    lists = [
        pltpu.make_async_copy(code_ref, code_smem, sem.at[1]),
        pltpu.make_async_copy(value_ref, value_smem, sem.at[2]),
    ]
    for move in lists:
        move.start()
    zeros = jnp.zeros((cells_y, LANES), F32)
    for p in range(RADIUS):
        grid_ref[p * cells_y : (p + 1) * cells_y, :] = zeros
        grid_ref[rim + own + p * cells_y : rim + own + (p + 1) * cells_y, :] = zeros
    for move in lists:
        move.wait()
    copy.wait()

    @pl.loop(0, partners)
    def _(p):
        @pl.loop(0, (code_smem[p, LANES - 1] + 3) // 4)
        def _(j):
            for k in range(4):
                code = code_smem[p, j * 4 + k]
                row = code // LANES
                amount = value_smem[p, j * 4 + k] * weight_ref[pl.ds(p * slots + code % LANES, 1), :]
                grid_ref[pl.ds(row, 1), :] = grid_ref[pl.ds(row, 1), :] + amount

    total = cells_x + 2 * RADIUS
    pick = picker()

    @pl.loop(0, cells_x, unroll=4)
    def _(x):
        plane = clipped(grid_ref[pl.ds(rim + x * cells_y, cells_y), :] - 0.5)
        flip_ref[x + RADIUS] = dot(pick, plane.astype(BF16), NT)

    for source_ref, base in ((low_ref, 0), (high_ref, RADIUS + cells_x)):
        @pl.loop(0, RADIUS, unroll=4)
        def _(p):
            plane = grid_ref[pl.ds((base + p) * cells_y, cells_y), :]
            deposited = dot(pick, plane.astype(BF16), NT)
            raw = jnp.concatenate(
                [
                    source_ref[p, (2 + k) * RADIUS : (3 + k) * RADIUS].astype(F32)
                    for k in range(cells_y // LANES)
                ],
                axis=1,
            )
            flip_ref[base + p] = clipped(raw + deposited)

    for source_ref, base in ((low_ref, 0), (high_ref, RADIUS + cells_x)):
        for p in range(RADIUS):
            for k, start in enumerate((0, cells_y - RADIUS)):
                at = (base + p) * cells_y + start
                edge = source_ref[p, k * RADIUS : (k + 1) * RADIUS].astype(F32)
                grid_ref[at : at + RADIUS, :] = grid_ref[at : at + RADIUS, :] + edge

    for k, start in enumerate((0, cells_y - RADIUS)):
        planes = []
        for e in range(total):
            at = e * cells_y + start
            bias = 0.5 if RADIUS <= e < RADIUS + cells_x else 0.0
            planes.append(clipped(grid_ref[at : at + RADIUS, :] - bias))
        for i, value in enumerate(running(planes, cells_x)):
            rows_out_ref[i, k * RADIUS : (k + 1) * RADIUS, :] = value

    for i, value in enumerate(running([flip_ref[e] for e in range(total)], cells_x)):
        rim_ref[i] = value.astype(BF16)


def edge_kernel(rows_ref, rim_ref, first_ref, last_ref):
    cells_x, double, cells_z = rows_ref.shape
    cells_y = rim_ref.shape[2]
    weights = cone(iota((cells_z, cells_z), 0) - iota((cells_z, cells_z), 1))
    weights = jnp.concatenate([weights, weights], axis=0)
    side = side_weights()
    rows = rows_ref[...].reshape(cells_x * double, cells_z)
    value = dot(jnp.concatenate(halves(rows), axis=1), weights)
    for x in range(cells_x):
        for k, out_ref in enumerate((first_ref, last_ref)):
            start = 0 if k == 0 else cells_y - LANES
            shift = 0 if k == 0 else LANES - RADIUS
            rim = rim_ref[x, :, start : start + LANES][:, shift : shift + RADIUS]
            at = x * double + k * RADIUS
            out_ref[x] = (value[at : at + RADIUS] + dot(rim, side, TN)).astype(BF16)


STEP = 8


def project_planes(
    scale_total, depth, places, smooth_ref, rim_ref, ends_ref, proj_ref, done
):
    _, _, cells_y = rim_ref.shape
    cells_z = proj_ref.shape[1]
    across = cone(iota((cells_y, cells_y), 0) - iota((cells_y, cells_y), 1))
    along = cone(iota((cells_z, cells_z), 0) - iota((cells_z, cells_z), 1))
    along = jnp.concatenate([along, side_weights()], axis=0)
    z = iota((1, cells_z), 1) + lax.axis_index("gz") * cells_z
    inside = jnp.zeros((1, cells_z), F32)
    for offset in range(-RADIUS, RADIUS + 1):
        good = (z + offset >= 0) & (z + offset < depth)
        inside = inside + jnp.where(good, float(TAPS - abs(offset)), 0.0)
    scale = 8.0 / (scale_total * inside)
    top = math.tanh(4.0)

    @pl.loop(0, places[1])
    def _(g):
        base = places[0] + g * places[2]
        rims = rim_ref[pl.ds(base, STEP)].reshape(STEP * RADIUS, cells_y)
        rims = dot(rims, across)
        for pair in range(STEP // 2):
            both = [smooth_ref[g * STEP + 2 * pair + k] for k in range(2)]
            both = dot(across, jnp.concatenate(both, axis=1)).astype(BF16)
            for k in range(2):
                x = base + 2 * pair + k
                at = (2 * pair + k) * RADIUS
                flipped = rims[at : at + RADIUS].T.astype(BF16)
                half = both[:, k * cells_z : (k + 1) * cells_z]
                value = dot(jnp.concatenate([half, flipped], axis=1), along)
                spot = pl.ds(pl.multiple_of(x * RADIUS, RADIUS), RADIUS)
                first = value[:RADIUS] + ends_ref[0, spot, :]
                last = value[cells_y - RADIUS :] + ends_ref[1, spot, :]
                value = jnp.concatenate([first, value[RADIUS : cells_y - RADIUS], last], axis=0)
                value = (top + jnp.tanh(value * scale)) * (1.0 / (2.0 * top))
                proj_ref[pl.ds(pl.multiple_of(x * cells_y, 8), cells_y), :] = value
        done(g)


def inner_kernel(
    scale_total, depth, grid_ref, rim_ref, before_ref, after_ref, proj_ref, ends_ref, smooth_ref
):
    cells_x, _, cells_y = rim_ref.shape
    cells_z = proj_ref.shape[1]
    many = cells_x * RADIUS
    row, column = iota((many, many), 0), iota((many, many), 1)
    same = row // RADIUS == column // RADIUS
    gap = row % RADIUS - column % RADIUS
    for rows_in_ref, distance, index in ((before_ref, gap + RADIUS, 0), (after_ref, gap - RADIUS, 1)):
        weights = jnp.where(same, cone(distance).astype(F32), 0.0).astype(BF16)
        ends_ref[index] = dot(weights, rows_in_ref[...].reshape(many, cells_z))
    count = cells_x - 2 * RADIUS
    chunk = 16

    @pl.loop(0, cells_y // chunk)
    def _(j):
        start = pl.multiple_of(j * chunk, chunk)
        planes = []
        for e in range(RADIUS, RADIUS + cells_x):
            at = pl.multiple_of(e * cells_y + start, chunk)
            planes.append(clipped(grid_ref[pl.ds(at, chunk), :] - 0.5))
        for i, value in enumerate(running(planes, count)):
            smooth_ref[i, pl.ds(start, chunk), :] = value.astype(BF16)

    project_planes(
        scale_total, depth, (RADIUS, count // STEP, STEP), smooth_ref, rim_ref, ends_ref,
        proj_ref, lambda g: None,
    )


def finish_kernel(
    scale_total, depth, inner_ref, own_ref, grid_ref, low_ref, high_ref, rim_ref, ends_ref,
    pay_ref, proj_ref, out_ref, ratio_ref, pad_ref, smooth_ref, picked_ref, rows_ref, sem, own_sem,
):
    cells_x, _, cells_y = rim_ref.shape
    cells_z = out_ref.shape[1]
    partners = pay_ref.shape[0]
    capacity = picked_ref.shape[0] // partners
    chunk = 16
    fetch = pltpu.make_async_copy(own_ref, rows_ref, own_sem)
    fetch.start()

    def send(first, count, index):
        rows = pl.ds(pl.multiple_of(first * cells_y, 8), count * cells_y)
        return pltpu.make_async_copy(proj_ref.at[rows], out_ref.at[rows], sem.at[index])

    inner_send = send(RADIUS, cells_x - 2 * RADIUS, 2)
    inner_send.start()
    for p in range(RADIUS):
        pad_ref[p, RADIUS : cells_y - RADIUS, :] = low_ref[p]
        pad_ref[RADIUS + p, RADIUS : cells_y - RADIUS, :] = high_ref[p]

    @pl.loop(0, cells_y // chunk)
    def _(j):
        start = pl.multiple_of(j * chunk, chunk)
        row = start + iota((chunk, 1), 0)
        main = (row >= RADIUS) & (row < cells_y - RADIUS)

        def own(e):
            at = pl.multiple_of(e * cells_y + start, chunk)
            return clipped(grid_ref[pl.ds(at, chunk), :] - 0.5)

        def outer(e, p):
            at = pl.multiple_of(e * cells_y + start, chunk)
            rim = pad_ref[p, pl.ds(start, chunk), :].astype(F32)
            return clipped(grid_ref[pl.ds(at, chunk), :] + jnp.where(main, rim, 0.0))

        planes = [outer(e, e) for e in range(RADIUS)]
        planes += [own(e) for e in range(RADIUS, 3 * RADIUS)]
        for i, value in enumerate(running(planes, RADIUS)):
            smooth_ref[i, pl.ds(start, chunk), :] = value.astype(BF16)
        planes = [own(e) for e in range(cells_x - RADIUS, cells_x + RADIUS)]
        planes += [outer(cells_x + RADIUS + p, RADIUS + p) for p in range(RADIUS)]
        for i, value in enumerate(running(planes, RADIUS)):
            smooth_ref[RADIUS + i, pl.ds(start, chunk), :] = value.astype(BF16)

    project_planes(
        scale_total, depth, (0, 2, cells_x - RADIUS), smooth_ref, rim_ref, ends_ref, proj_ref,
        lambda g: send(g * (cells_x - RADIUS), RADIUS, g).start(),
    )
    fetch.wait()

    @pl.loop(0, partners)
    def _(p):
        for s in range(capacity):
            row = rows_ref[p, s]
            picked_ref[pl.ds(p * capacity + s, 1), :] = proj_ref[pl.ds(row, 1), :]

    ones = jnp.ones((8, cells_z), BF16)
    group = LANES // capacity

    @pl.loop(0, partners * capacity // LANES)
    def _(c):
        w = pay_ref[pl.ds(c * group, group), :capacity, :].reshape(LANES, cells_z)
        picked = picked_ref[pl.ds(pl.multiple_of(c * LANES, LANES), LANES), :]
        high, low = halves(w.astype(F32) * picked)
        amount = dot(ones, high, NT) + dot(ones, low, NT)
        ratio_ref[pl.ds(c, 1), :] = (amount / dot(ones, w, NT))[:1]

    for g in range(2):
        send(g * (cells_x - RADIUS), RADIUS, g).wait()
    inner_send.wait()


def back_kernel(counts_ref, elements_ref, ratio_ref, out_ref):
    tiles, capacity = elements_ref.shape
    high_count = out_ref.shape[0]
    group = min(tiles, 16)
    wide = group * capacity
    out_ref[...] = jnp.zeros(out_ref.shape, F32)

    @pl.loop(0, tiles // group)
    def _(g):
        start = pl.multiple_of(g * group, group)
        element = elements_ref[pl.ds(start, group), :]
        tile = iota((group, tiles), 0) + start == iota((group, tiles), 1)
        counts = jnp.where(tile, counts_ref[...].astype(F32), 0.0)
        counts = jnp.sum(counts, axis=1, keepdims=True)
        live = iota((group, capacity), 1).astype(F32) < counts
        ratio = jnp.where(live, ratio_ref[pl.ds(start, group), :], 0.0)
        first, _ = halves(ratio)
        second, third = halves(ratio - first.astype(F32))
        parts = [(element // LANES).astype(F32), (element % LANES).astype(F32)]
        parts += [part.astype(F32) for part in (first, second, third)]
        spread = onehot(iota((capacity, wide), 1) % capacity == iota((capacity, wide), 0))
        own = iota((group, wide), 1) // capacity == iota((group, wide), 0)
        rows = []
        for part in parts:
            part = jnp.where(own, dot(part.astype(BF16), spread), 0.0)
            rows.append(jnp.sum(part, axis=0, keepdims=True))
        lane = onehot(iota((LANES, wide), 0).astype(F32) == rows[1])
        mine = iota((high_count, wide), 0).astype(F32) == rows[0]
        total = jnp.zeros(out_ref.shape, F32)
        for part in rows[2:]:
            total = total + dot(jnp.where(mine, part, 0.0).astype(BF16), lane, NT)
        out_ref[...] = out_ref[...] + total


def update(
    design,
    forward_edges,
    adjoint_edges,
    edge_basis,
    quad_weights,
    slot_weights,
    slot_elements,
    slot_blocks,
    slot_counts,
):
    cells_x, cells_y, cells_z = design.shape
    tiles, capacity = slot_elements.shape
    n_tx, n_ty, n_gz = (lax.axis_size(a) for a in ("tx", "ty", "gz"))
    if cells_z != LANES or cells_y != 256 or n_gz != 2:
        raise NotImplementedError
    slots = 3 * capacity
    edge_count, elements = forward_edges.shape[1:]
    rows_ext = (cells_x + 2 * RADIUS) * cells_y
    whole = pl.BlockSpec(memory_space=VMEM)
    anywhere = pl.BlockSpec(memory_space=pltpu.HBM)
    shape = jax.ShapeDtypeStruct
    stay = lambda x: pltpu.with_memory_space_constraint(x, pltpu.HBM)
    params = lambda mib: pltpu.CompilerParams(vmem_limit_bytes=mib << 20)

    inner = cells_y - 2 * RADIUS
    edge_rows = 2 * RADIUS + RADIUS * cells_y // LANES
    payload = pl.pallas_call(
        functools.partial(pack_kernel, n_ty, cells_x, cells_y),
        out_shape=shape((tiles, slots + 8, LANES), BF16),
        in_specs=[anywhere] * 8,
        out_specs=whole,
        scratch_shapes=[
            VMEM(edge_basis.shape[::-1], F32),
            VMEM((edge_count, 2, elements), F32),
            VMEM((edge_count, 2, elements), F32),
            VMEM(slot_weights.shape, BF16),
            VMEM(slot_elements.shape, jnp.int32),
            VMEM(slot_blocks.shape, jnp.int32),
            SMEM(slot_counts.shape, jnp.int32),
            SMEM(quad_weights.shape, F32),
            VMEM((4, tiles, LANES), F32),
            pltpu.SemaphoreType.DMA((8,)),
        ],
        compiler_params=params(24),
        name="pack",
    )(
        stay(slot_counts),
        stay(quad_weights),
        stay(edge_basis.T),
        stay(forward_edges.transpose(1, 0, 2)),
        stay(adjoint_edges.transpose(1, 0, 2)),
        stay(slot_weights),
        stay(slot_elements),
        stay(slot_blocks),
    )

    arrived = lax.all_to_all(payload, ("tx", "ty"), split_axis=0, concat_axis=0, tiled=True)
    up = [(i, (i + 1) % n_tx) for i in range(n_tx)]
    down = [(t, s) for s, t in up]

    def cast(kernel, rows, token):
        strip = shape((RADIUS, rows, LANES), BF16)
        return pl.pallas_call(
            kernel,
            out_shape=(strip, strip),
            in_specs=[anywhere, anywhere],
            out_specs=(whole, whole),
            scratch_shapes=[
                VMEM((2 * RADIUS, cells_y, cells_z), F32),
                pltpu.SemaphoreType.DMA((2,)),
            ],
            compiler_params=params(16),
        )(stay(design), token)

    up_edge, down_edge = cast(cast_edge_kernel, edge_rows, stay(payload))
    low_edge = lax.ppermute(up_edge, "tx", up)
    high_edge = lax.ppermute(down_edge, "tx", down)
    up_main, down_main = cast(cast_main_kernel, inner, up_edge)
    low_main = lax.ppermute(up_main, "tx", up)
    high_main = lax.ppermute(down_main, "tx", down)

    grid, edge_smooth, rim, rows_own = pl.pallas_call(
        functools.partial(deposit_kernel, cells_y, slots),
        out_shape=(
            shape((rows_ext, cells_z), F32),
            shape((cells_x, 2 * RADIUS, cells_z), F32),
            shape((cells_x, RADIUS, cells_y), BF16),
            shape((tiles, LANES), jnp.int32),
        ),
        in_specs=[anywhere] + [whole] * 3,
        out_specs=(whole,) * 4,
        scratch_shapes=[
            VMEM((cells_x + 2 * RADIUS, RADIUS, cells_y), F32),
            VMEM((tiles * slots, LANES), F32),
            VMEM((tiles, LANES), jnp.int32),
            VMEM((tiles, LANES), F32),
            SMEM((tiles, LANES), jnp.int32),
            SMEM((tiles, LANES), F32),
            pltpu.SemaphoreType.DMA((3,)),
        ],
        compiler_params=params(16),
        name="deposit",
    )(stay(design.reshape(cells_x * cells_y, cells_z)), low_edge, high_edge, arrived)

    rim = lax.ppermute(rim, "gz", [(0, 1), (1, 0)])
    edge = shape((cells_x, RADIUS, cells_z), BF16)
    first, last = pl.pallas_call(
        edge_kernel,
        out_shape=(edge, edge),
        in_specs=[whole, whole],
        out_specs=(whole, whole),
        compiler_params=params(16),
        name="edges",
    )(edge_smooth, rim)
    up = [(i, (i + 1) % n_ty) for i in range(n_ty)]
    down = [(t, s) for s, t in up]
    before = lax.ppermute(last, "ty", up)
    after = lax.ppermute(first, "ty", down)

    flat = shape((cells_x * cells_y, cells_z), F32)
    constants = (float(TAPS**4), n_gz * cells_z)
    call = pl.pallas_call(
        functools.partial(inner_kernel, *constants),
        out_shape=(flat, shape((2, cells_x * RADIUS, cells_z), F32)),
        in_specs=[whole] * 4,
        out_specs=(whole, whole),
        scratch_shapes=[VMEM((cells_x - 2 * RADIUS, cells_y, cells_z), BF16)],
        compiler_params=params(16),
        name="inner",
    )
    partial, ends = call(grid, rim, before, after)
    _, projected, ratios = pl.pallas_call(
        functools.partial(finish_kernel, *constants),
        out_shape=(flat, flat, shape((tiles * capacity // LANES, LANES), F32)),
        in_specs=[whole] * 8,
        out_specs=(whole, anywhere, whole),
        scratch_shapes=[
            VMEM((2 * RADIUS, cells_y, cells_z), BF16),
            VMEM((2 * RADIUS, cells_y, cells_z), BF16),
            VMEM((tiles * capacity, cells_z), F32),
            SMEM((tiles, LANES), jnp.int32),
            pltpu.SemaphoreType.DMA((3,)),
            pltpu.SemaphoreType.DMA,
        ],
        input_output_aliases={0: 0},
        compiler_params=params(16),
        name="finish",
    )(partial, rows_own, grid, low_main, high_main, rim, ends, arrived)

    ratios = ratios.reshape(tiles, capacity)
    ratios = lax.all_to_all(ratios, ("tx", "ty"), split_axis=0, concat_axis=0, tiled=True)
    density = pl.pallas_call(
        back_kernel,
        out_shape=shape((elements // LANES, LANES), F32),
        in_specs=[whole] * 3,
        out_specs=whole,
        compiler_params=params(16),
        name="to_elements",
    )(slot_counts, slot_elements, ratios)
    return projected.reshape(design.shape), density.reshape(elements)


def solution(mesh):
    in_specs = (
        P("tx", "ty", "gz"),
        P(None, None, ("tx", "ty", "gz")),
        P(None, None, ("tx", "ty", "gz")),
        P(),
        P(),
        P(("tx", "ty", "gz"), None, None),
        P(("tx", "ty", "gz"), None),
        P(("tx", "ty", "gz"), None),
        P(("tx", "ty", "gz"), None),
    )
    out_specs = (P("tx", "ty", "gz"), P(("tx", "ty", "gz")))
    return jax.shard_map(update, mesh=mesh, in_specs=in_specs, out_specs=out_specs, check_vma=False)
```

```python
import functools
import math

import jax
import jax.numpy as jnp
from jax import lax
from jax.experimental import pallas as pl
from jax.experimental.pallas import tpu as pltpu
from jax.sharding import PartitionSpec as P


RADIUS = 8
LANES = 128
TAPS = RADIUS + 1
STEP = 8
NEAR = RADIUS // 2
GROUP = 6
F32 = jnp.float32
BF16 = jnp.bfloat16
SMEM = pltpu.SMEM
VMEM = pltpu.VMEM
NT = ((1,), (1,))


def iota(shape, dim):
    return lax.broadcasted_iota(jnp.int32, shape, dim)


def onehot(mask):
    return mask.astype(F32).astype(BF16)


def cone(distance):
    return jnp.maximum(TAPS - jnp.abs(distance), 0).astype(F32).astype(BF16)


def halves(x):
    high = x.astype(BF16)
    return high, (x - high.astype(F32)).astype(BF16)


def dot(a, b, contract=((1,), (0,)), precision=None):
    return lax.dot_general(
        a, b, (contract, ((), ())), preferred_element_type=F32, precision=precision
    )


def picker():
    first = jnp.where(lax.axis_index("gz") == 0, LANES - RADIUS, 0)
    return onehot(iota((RADIUS, LANES), 1) == iota((RADIUS, LANES), 0) + first)


def side_weights():
    first = jnp.where(lax.axis_index("gz") == 0, LANES, -RADIUS)
    return cone(iota((RADIUS, LANES), 0) + first - iota((RADIUS, LANES), 1))


def running(planes, length):
    add = lambda a, b: a + b
    box = [functools.reduce(add, planes[:TAPS])]
    for k in range(length + RADIUS - 1):
        box.append(box[-1] + (planes[k + TAPS] - planes[k]))
    total = functools.reduce(add, box[:TAPS])
    out = [total]
    for i in range(length - 1):
        total = total + (box[i + TAPS] - box[i])
        out.append(total)
    return out


def clipped(x):
    return jnp.clip(x, -0.5, 0.5)


def pack_kernel(
    n_ty, cells_x, cells_y, counts_hbm, quad_hbm, basis_hbm, forward_hbm, adjoint_hbm, weights_hbm,
    elements_hbm, blocks_hbm, pay_ref, basis_ref, forward_ref, adjoint_ref, weights_ref,
    elements_ref, blocks_ref, counts_ref, quad_ref, code_ref, sem,
):
    sources = (forward_hbm, adjoint_hbm, basis_hbm, elements_hbm, blocks_hbm, weights_hbm)
    sources += (counts_hbm, quad_hbm)
    targets = (forward_ref, adjoint_ref, basis_ref, elements_ref, blocks_ref, weights_ref)
    targets += (counts_ref, quad_ref)
    loads = [
        pltpu.make_async_copy(source, target, sem.at[i])
        for i, (source, target) in enumerate(zip(sources, targets))
    ]
    for load in loads:
        load.start()
    tiles, capacity = elements_ref.shape
    points = quad_ref.shape[0]
    highest = lax.Precision.HIGHEST
    for load in loads:
        load.wait()

    terms, edges = 2 * forward_ref.shape[0], forward_ref.shape[0]
    point = iota((1, 3 * points), 1) % points
    quad = jnp.zeros((1, 3 * points), F32)
    for q in range(points):
        quad = quad + jnp.where(point == q, quad_ref[q], 0.0)
    twice = (iota((terms, edges), 0) // 2 == iota((terms, edges), 1)).astype(F32)
    basis = dot(twice, basis_ref[...], precision=highest)
    gram = dot(basis * quad, basis, NT, precision=highest)
    row, column = iota((terms, terms), 0), iota((terms, terms), 1)
    gram = jnp.where(row % 2 == 0, gram, -gram)
    gram = jnp.where(row % 2 == column % 2, gram, 0.0)
    adjoint = jnp.concatenate([adjoint_ref[k] for k in range(edges)], axis=0)
    forward = jnp.concatenate([forward_ref[k] for k in range(edges)], axis=0)
    sens = jnp.sum(forward * dot(gram, adjoint, precision=highest), axis=0, keepdims=True)
    groups = sens.shape[1] // LANES
    sens = jnp.concatenate([sens[:, g * LANES : (g + 1) * LANES] for g in range(groups)], axis=0)
    first, _ = halves(sens)
    second, third = halves(sens - first.astype(F32))
    parts = jnp.concatenate([first, second, third], axis=0)

    element, block = elements_ref[...], blocks_ref[...]
    codes = [
        element // LANES,
        element % LANES,
        block // cells_y + RADIUS,
        block % cells_y,
    ]
    place = iota((capacity, LANES), 1) - iota((capacity, LANES), 0)
    for index, code in enumerate(codes):
        code = code.astype(F32).astype(BF16)
        total = jnp.zeros((tiles, LANES), F32)
        for order, d in enumerate((0, -1, 1)):
            moved = dot(code, onehot(place == order * capacity))
            shift = (d * n_ty) % tiles
            if shift:
                moved = jnp.concatenate([moved[shift:], moved[:shift]], axis=0)
            if index == 2 and d:
                group = iota((tiles, LANES), 1) // capacity
                moved = moved + jnp.where(group == order, float(d * cells_x), 0.0)
            total = total + moved
        code_ref[index] = total

    @pl.loop(0, tiles, unroll=min(tiles, 16))
    def _(t):
        high, low, plane, line = (code_ref[index, pl.ds(t, 1), :] for index in range(4))
        lane = iota((1, LANES), 1)
        live = jnp.zeros((1, LANES), jnp.bool_)
        sources = []
        for order, d in enumerate((0, -1, 1)):
            source = lax.rem(t + (d * n_ty) % tiles, tiles)
            sources.append(source)
            at = lane - order * capacity
            live = live | ((at >= 0) & (at < capacity) & (at < counts_ref[0, source]))
        hit = onehot(iota((LANES, LANES), 0).astype(F32) == low)
        found = dot(parts, hit)
        found = (found[:groups] + found[groups : 2 * groups]) + found[2 * groups :]
        mine = iota((groups, LANES), 0).astype(F32) == high
        value = jnp.sum(jnp.where(mine, found, 0.0), axis=0, keepdims=True)
        value = jnp.where(live, value, 0.0).astype(BF16).astype(F32) * -0.5
        kind = iota((8, LANES), 0)
        meta = jnp.where(kind == 0, plane, jnp.where(kind == 1, line, value))
        meta = jnp.where(kind < 3, meta, 0.0)
        for order, source in enumerate(sources):
            pay_ref[t, order * capacity : (order + 1) * capacity, :] = weights_ref[source]
        pay_ref[t, 3 * capacity :, :] = meta.astype(BF16)


def strips(design_ref, strip_ref, sem):
    cells_x = design_ref.shape[0]
    return [
        pltpu.make_async_copy(
            design_ref.at[pl.ds(start, RADIUS)], strip_ref.at[pl.ds(side * RADIUS, RADIUS)],
            sem.at[side],
        )
        for side, start in enumerate((0, cells_x - RADIUS))
    ]


def cast_kernel(
    design_ref, token_ref, up_ref, down_ref, up_near_ref, down_near_ref, up_far_ref, down_far_ref,
    strip_ref, sem,
):
    cells_y = design_ref.shape[1]
    edge_rows = 2 * RADIUS + RADIUS * cells_y // LANES
    copies = strips(design_ref, strip_ref, sem)
    for copy in copies:
        copy.start()
    pick = picker()
    by_side = ((down_ref, down_near_ref, down_far_ref), (up_ref, up_far_ref, up_near_ref))
    for side, targets in enumerate(by_side):
        copies[side].wait()
        for p in range(RADIUS):
            plane = strip_ref[side * RADIUS + p] - 0.5
            targets[1 + p // NEAR][p % NEAR] = plane[RADIUS : cells_y - RADIUS].astype(BF16)
            flipped = dot(pick, plane.astype(BF16), NT)
            pieces = [plane[:RADIUS], plane[cells_y - RADIUS :]]
            pieces += [flipped[:, k * LANES : (k + 1) * LANES] for k in range(cells_y // LANES)]
            pieces = jnp.concatenate(pieces, axis=0).astype(BF16)
            targets[0][p * edge_rows : (p + 1) * edge_rows, :] = pieces


def prefix_kernel(token_ref, out_ref):
    out_ref[...] = onehot(iota((LANES, LANES), 0) <= iota((LANES, LANES), 1))


def deposit_kernel(
    cells_y, slots, design_ref, low_ref, high_ref, pay_ref, prefix_ref, grid_ref, rows_out_ref,
    small_ref, rim_ref, own_ref, flip_ref, weight_ref, code_ref, value_ref, code_smem, value_smem, sem,
):
    cells_x = design_ref.shape[0] // cells_y
    partners = pay_ref.shape[0]
    rim = RADIUS * cells_y
    own = cells_x * cells_y
    edge_rows = 2 * RADIUS + RADIUS * cells_y // LANES
    copy = pltpu.make_async_copy(design_ref, grid_ref.at[pl.ds(rim, own)], sem.at[0])
    copy.start()

    lane = iota((1, LANES), 1)
    upper = prefix_ref[...]

    def decode(p):
        weight_ref[pl.ds(pl.multiple_of(p * slots, 16), slots), :] = pay_ref[p, :slots, :].astype(F32)
        meta = pay_ref[p, slots : slots + 8, :].astype(F32)
        plane, line, value = meta[0:1], meta[1:2], meta[2:3]
        own_ref[pl.ds(p, 1), :] = ((plane - float(RADIUS)) * float(cells_y) + line).astype(jnp.int32)
        used = (plane >= 0.0) & (plane < float(cells_x + 2 * RADIUS)) & (value != 0.0)
        used = jnp.where(used & (lane < slots), 1.0, 0.0)
        order = dot(jnp.broadcast_to(used, (8, LANES)).astype(BF16), upper)[:1]
        place = jnp.where(used > 0.0, order - 1.0, -1.0)
        hit = onehot(iota((LANES, LANES), 0).astype(F32) == place)
        kind = iota((8, LANES), 0)
        meta = jnp.where(kind == 3, lane.astype(F32), jnp.where(kind < 3, meta, 0.0))
        moved = dot(meta.astype(BF16), hit, NT)
        code = (moved[0:1] * float(cells_y) + moved[1:2]) * float(LANES) + moved[3:4]
        code = jnp.where(lane == LANES - 1, order[:, LANES - 1 :], code)
        code_ref[pl.ds(p, 1), :] = code.astype(jnp.int32)
        value_ref[pl.ds(p, 1), :] = moved[2:3]

    half = partners // 2
    lists = []
    for h in range(2):
        part = pl.ds(h * half, half)
        pl.loop(h * half, (h + 1) * half, unroll=min(half, 8))(decode)
        moves = [
            pltpu.make_async_copy(code_ref.at[part], code_smem.at[part], sem.at[1 + 2 * h]),
            pltpu.make_async_copy(value_ref.at[part], value_smem.at[part], sem.at[2 + 2 * h]),
        ]
        for move in moves:
            move.start()
        lists.append(moves)
    zeros = jnp.zeros((cells_y, LANES), F32)
    for p in range(RADIUS):
        grid_ref[p * cells_y : (p + 1) * cells_y, :] = zeros
        grid_ref[rim + own + p * cells_y : rim + own + (p + 1) * cells_y, :] = zeros
    copy.wait()

    def scatter(p):
        @pl.loop(0, (code_smem[p, LANES - 1] + GROUP - 1) // GROUP)
        def _(j):
            codes = [code_smem[p, j * GROUP + k] for k in range(GROUP)]
            spots = [code // LANES for code in codes]
            amounts = [
                value_smem[p, j * GROUP + k] * weight_ref[pl.ds(p * slots + codes[k] % LANES, 1), :]
                for k in range(GROUP)
            ]
            olds = [grid_ref[pl.ds(spot, 1), :] for spot in spots]
            for k in range(GROUP):
                amount = amounts[k]
                for i in range(k):
                    amount = amount + jnp.where(spots[i] == spots[k], 1.0, 0.0) * amounts[i]
                grid_ref[pl.ds(spots[k], 1), :] = olds[k] + amount

    for h in range(2):
        for move in lists[h]:
            move.wait()
        pl.loop(h * half, (h + 1) * half)(scatter)

    total = cells_x + 2 * RADIUS
    pick = picker()

    @pl.loop(0, cells_x, unroll=16)
    def _(x):
        plane = clipped(grid_ref[pl.ds(rim + x * cells_y, cells_y), :] - 0.5)
        flip_ref[x + RADIUS] = dot(pick, plane.astype(BF16), NT)

    for source_ref, base in ((low_ref, 0), (high_ref, RADIUS + cells_x)):
        for p in range(RADIUS):
            plane = grid_ref[pl.ds((base + p) * cells_y, cells_y), :]
            deposited = dot(pick, plane.astype(BF16), NT)
            raw = jnp.concatenate(
                [
                    source_ref[pl.ds(p * edge_rows + (2 + k) * RADIUS, RADIUS), :].astype(F32)
                    for k in range(cells_y // LANES)
                ],
                axis=1,
            )
            flip_ref[base + p] = clipped(raw + deposited)

    for source_ref, base in ((low_ref, 0), (high_ref, RADIUS + cells_x)):
        for p in range(RADIUS):
            for k, start in enumerate((0, cells_y - RADIUS)):
                at = (base + p) * cells_y + start
                edge = source_ref[p * edge_rows + k * RADIUS : p * edge_rows + (k + 1) * RADIUS, :]
                edge = edge.astype(F32)
                grid_ref[at : at + RADIUS, :] = grid_ref[at : at + RADIUS, :] + edge

    for k, start in enumerate((0, cells_y - RADIUS)):
        planes = []
        for e in range(total):
            at = e * cells_y + start
            bias = 0.5 if RADIUS <= e < RADIUS + cells_x else 0.0
            planes.append(clipped(grid_ref[at : at + RADIUS, :] - bias))
        for i, value in enumerate(running(planes, cells_x)):
            rows_out_ref[i, k * RADIUS : (k + 1) * RADIUS, :] = value

    double = 2 * RADIUS
    rows = rows_out_ref[...].reshape(cells_x * double, LANES).astype(BF16)
    first = jnp.where(lax.axis_index("gz") == 0, LANES - RADIUS, 0)
    tiled = onehot(iota((LANES, LANES), 0) == iota((LANES, LANES), 1) % RADIUS + first)
    shape = (cells_x * double, LANES)
    mine = iota(shape, 0) % double == iota(shape, 1) // RADIUS
    small = jnp.where(mine, dot(rows, tiled), 0.0).reshape(cells_x, double, LANES)
    small_ref[...] = jnp.sum(small, axis=1).astype(BF16)

    for i, value in enumerate(running([flip_ref[e] for e in range(total)], cells_x)):
        rim_ref[i] = value.astype(BF16)


def edge_kernel(rows_ref, small_ref, first_ref, last_ref):
    cells_x, double, cells_z = rows_ref.shape
    weights = cone(iota((cells_z, cells_z), 0) - iota((cells_z, cells_z), 1))
    weights = jnp.concatenate([weights, weights], axis=0)
    side = jnp.concatenate([side_weights()] * double, axis=0)
    rows = rows_ref[...].reshape(cells_x * double, cells_z)
    shape = (cells_x * double, LANES)
    repeat = onehot(iota((shape[0], cells_x), 0) // double == iota((shape[0], cells_x), 1))
    mine = iota(shape, 0) % double == iota(shape, 1) // RADIUS
    spread = jnp.where(mine, dot(repeat, small_ref[...]), 0.0).astype(BF16)
    value = dot(jnp.concatenate(halves(rows), axis=1), weights) + dot(spread, side)
    value = value.astype(BF16)
    for x in range(cells_x):
        first_ref[x] = value[x * double : x * double + RADIUS]
        last_ref[x] = value[x * double + RADIUS : (x + 1) * double]


def project_planes(
    scale_total, depth, places, step, smooth_ref, rim_ref, ends_ref, proj_ref, done
):
    _, _, cells_y = rim_ref.shape
    cells_z = proj_ref.shape[1]
    across = cone(iota((cells_y, cells_y), 0) - iota((cells_y, cells_y), 1))
    along = cone(iota((cells_z, cells_z), 0) - iota((cells_z, cells_z), 1))
    along = jnp.concatenate([along, side_weights()], axis=0)
    z = iota((1, cells_z), 1) + lax.axis_index("gz") * cells_z
    inside = jnp.zeros((1, cells_z), F32)
    for offset in range(-RADIUS, RADIUS + 1):
        good = (z + offset >= 0) & (z + offset < depth)
        inside = inside + jnp.where(good, float(TAPS - abs(offset)), 0.0)
    scale = 8.0 / (scale_total * inside)
    top = math.tanh(4.0)

    @pl.loop(0, places[1], unroll=STEP // step)
    def _(g):
        base = places[0] + g * places[2]
        rims = rim_ref[pl.ds(base, step)].reshape(step * RADIUS, cells_y)
        rims = dot(rims, across)
        for pair in range(step // 2):
            both = [smooth_ref[g * step + 2 * pair + k] for k in range(2)]
            both = dot(across, jnp.concatenate(both, axis=1)).astype(BF16)
            for k in range(2):
                x = base + 2 * pair + k
                at = (2 * pair + k) * RADIUS
                flipped = rims[at : at + RADIUS].T.astype(BF16)
                half = both[:, k * cells_z : (k + 1) * cells_z]
                value = dot(jnp.concatenate([half, flipped], axis=1), along)
                spot = pl.ds(pl.multiple_of(x * RADIUS, RADIUS), RADIUS)
                first = value[:RADIUS] + ends_ref[0, spot, :]
                last = value[cells_y - RADIUS :] + ends_ref[1, spot, :]
                value = jnp.concatenate([first, value[RADIUS : cells_y - RADIUS], last], axis=0)
                value = (top + jnp.tanh(value * scale)) * (1.0 / (2.0 * top))
                proj_ref[pl.ds(pl.multiple_of(x * cells_y, 8), cells_y), :] = value
        done(g)


def smooth_x(grid_ref, pad_ref, low, high, start, rows, main):
    cells_y = pad_ref.shape[1]
    cells_x = grid_ref.shape[0] // cells_y - 2 * RADIUS

    def plane(e):
        at = pl.multiple_of(e * cells_y + start, rows)
        value = grid_ref[pl.ds(at, rows), :]
        if RADIUS <= e < RADIUS + cells_x:
            return clipped(value - 0.5)
        p = e if e < RADIUS else e - cells_x
        rim = pad_ref[p, pl.ds(start, rows), :].astype(F32)
        return clipped(value + jnp.where(main, rim, 0.0))

    return running([plane(e) for e in range(low, high + 2 * RADIUS)], high - low)


def main_rows(start, rows, cells_y):
    row = start + iota((rows, 1), 0)
    return (row >= RADIUS) & (row < cells_y - RADIUS)


def inner_kernel(
    scale_total, depth, grid_ref, low_ref, high_ref, rim_ref, before_ref, after_ref, proj_ref,
    ends_ref, pad_ref, smooth_ref,
):
    cells_x, _, cells_y = rim_ref.shape
    cells_z = proj_ref.shape[1]
    many = cells_x * RADIUS
    row, column = iota((many, many), 0), iota((many, many), 1)
    same = row // RADIUS == column // RADIUS
    gap = row % RADIUS - column % RADIUS
    for rows_in_ref, distance, index in ((before_ref, gap + RADIUS, 0), (after_ref, gap - RADIUS, 1)):
        weights = jnp.where(same, cone(distance).astype(F32), 0.0).astype(BF16)
        ends_ref[index] = dot(weights, rows_in_ref[...].reshape(many, cells_z))
    count = cells_x - RADIUS
    chunk = 16
    for p in range(NEAR):
        pad_ref[NEAR + p, RADIUS : cells_y - RADIUS, :] = low_ref[p]
        pad_ref[RADIUS + p, RADIUS : cells_y - RADIUS, :] = high_ref[p]

    @pl.loop(0, cells_y // chunk)
    def _(j):
        start = pl.multiple_of(j * chunk, chunk)
        main = main_rows(start, chunk, cells_y)
        values = smooth_x(grid_ref, pad_ref, NEAR, cells_x - NEAR, start, chunk, main)
        for i, value in enumerate(values):
            smooth_ref[i, pl.ds(start, chunk), :] = value.astype(BF16)

    project_planes(
        scale_total, depth, (NEAR, count // STEP, STEP), STEP, smooth_ref, rim_ref, ends_ref,
        proj_ref, lambda g: None,
    )


def finish_kernel(
    scale_total, depth, inner_ref, own_ref, grid_ref, low_near_ref, high_near_ref, low_far_ref,
    high_far_ref, rim_ref, ends_ref, pay_ref, proj_ref, out_ref, ratio_ref, pad_ref, smooth_ref,
    picked_ref, rows_ref, sem, own_sem,
):
    cells_x, _, cells_y = rim_ref.shape
    cells_z = out_ref.shape[1]
    partners = pay_ref.shape[0]
    capacity = picked_ref.shape[0] // partners
    chunk = 16
    fetch = pltpu.make_async_copy(own_ref, rows_ref, own_sem)
    fetch.start()

    def send(first, count, index):
        rows = pl.ds(pl.multiple_of(first * cells_y, 8), count * cells_y)
        return pltpu.make_async_copy(proj_ref.at[rows], out_ref.at[rows], sem.at[index])

    inner_send = send(NEAR, cells_x - RADIUS, 2)
    inner_send.start()
    sources = (low_far_ref, low_near_ref, high_near_ref, high_far_ref)
    for index, source_ref in enumerate(sources):
        for p in range(NEAR):
            pad_ref[index * NEAR + p, RADIUS : cells_y - RADIUS, :] = source_ref[p]

    @pl.loop(0, cells_y // chunk)
    def _(j):
        start = pl.multiple_of(j * chunk, chunk)
        main = main_rows(start, chunk, cells_y)
        values = smooth_x(grid_ref, pad_ref, 0, NEAR, start, chunk, main)
        values += smooth_x(grid_ref, pad_ref, cells_x - NEAR, cells_x, start, chunk, main)
        for i, value in enumerate(values):
            smooth_ref[i, pl.ds(start, chunk), :] = value.astype(BF16)

    last = cells_x - NEAR
    project_planes(
        scale_total, depth, (0, 2, last), NEAR, smooth_ref, rim_ref, ends_ref, proj_ref,
        lambda g: send(g * last, NEAR, g).start(),
    )
    fetch.wait()

    @pl.loop(0, partners)
    def _(p):
        for s in range(capacity):
            row = rows_ref[p, s]
            picked_ref[pl.ds(p * capacity + s, 1), :] = proj_ref[pl.ds(row, 1), :]

    ones = jnp.ones((8, cells_z), BF16)
    group = LANES // capacity

    @pl.loop(0, partners * capacity // LANES)
    def _(c):
        w = pay_ref[pl.ds(c * group, group), :capacity, :].reshape(LANES, cells_z)
        picked = picked_ref[pl.ds(pl.multiple_of(c * LANES, LANES), LANES), :]
        high, low = halves(w.astype(F32) * picked)
        amount = dot(ones, high, NT) + dot(ones, low, NT)
        ratio_ref[pl.ds(c, 1), :] = (amount / dot(ones, w, NT))[:1]

    for g in range(2):
        send(g * last, NEAR, g).wait()
    inner_send.wait()


def back_kernel(counts_ref, elements_ref, ratio_ref, out_ref):
    tiles, capacity = elements_ref.shape
    high_count = out_ref.shape[0]
    group = min(tiles, 16)
    wide = group * capacity
    out_ref[...] = jnp.zeros(out_ref.shape, F32)

    @pl.loop(0, tiles // group)
    def _(g):
        start = pl.multiple_of(g * group, group)
        element = elements_ref[pl.ds(start, group), :]
        tile = iota((group, tiles), 0) + start == iota((group, tiles), 1)
        counts = jnp.where(tile, counts_ref[...].astype(F32), 0.0)
        counts = jnp.sum(counts, axis=1, keepdims=True)
        live = iota((group, capacity), 1).astype(F32) < counts
        ratio = jnp.where(live, ratio_ref[pl.ds(start, group), :], 0.0)
        first, _ = halves(ratio)
        second, third = halves(ratio - first.astype(F32))
        parts = [(element // LANES).astype(F32), (element % LANES).astype(F32)]
        parts += [part.astype(F32) for part in (first, second, third)]
        spread = onehot(iota((capacity, wide), 1) % capacity == iota((capacity, wide), 0))
        own = iota((group, wide), 1) // capacity == iota((group, wide), 0)
        rows = []
        for part in parts:
            part = jnp.where(own, dot(part.astype(BF16), spread), 0.0)
            rows.append(jnp.sum(part, axis=0, keepdims=True))
        lane = onehot(iota((LANES, wide), 0).astype(F32) == rows[1])
        mine = iota((high_count, wide), 0).astype(F32) == rows[0]
        total = jnp.zeros(out_ref.shape, F32)
        for part in rows[2:]:
            total = total + dot(jnp.where(mine, part, 0.0).astype(BF16), lane, NT)
        out_ref[...] = out_ref[...] + total


def update(
    design,
    forward_edges,
    adjoint_edges,
    edge_basis,
    quad_weights,
    slot_weights,
    slot_elements,
    slot_blocks,
    slot_counts,
):
    cells_x, cells_y, cells_z = design.shape
    tiles, capacity = slot_elements.shape
    n_tx, n_ty, n_gz = (lax.axis_size(a) for a in ("tx", "ty", "gz"))
    if cells_z != LANES or cells_y != 256 or n_gz != 2:
        raise NotImplementedError
    slots = 3 * capacity
    edge_count, elements = forward_edges.shape[1:]
    rows_ext = (cells_x + 2 * RADIUS) * cells_y
    whole = pl.BlockSpec(memory_space=VMEM)
    anywhere = pl.BlockSpec(memory_space=pltpu.HBM)
    shape = jax.ShapeDtypeStruct
    stay = lambda x: pltpu.with_memory_space_constraint(x, pltpu.HBM)
    params = lambda mib: pltpu.CompilerParams(vmem_limit_bytes=mib << 20)

    inner = cells_y - 2 * RADIUS
    edge_rows = 2 * RADIUS + RADIUS * cells_y // LANES
    up = [(i, (i + 1) % n_tx) for i in range(n_tx)]
    down = [(t, s) for s, t in up]

    call = pl.pallas_call(
        functools.partial(pack_kernel, n_ty, cells_x, cells_y),
        out_shape=shape((tiles, slots + 8, LANES), BF16),
        in_specs=[anywhere] * 8,
        out_specs=whole,
        scratch_shapes=[
            VMEM(edge_basis.shape[::-1], F32),
            VMEM((edge_count, 2, elements), F32),
            VMEM((edge_count, 2, elements), F32),
            VMEM(slot_weights.shape, BF16),
            VMEM(slot_elements.shape, jnp.int32),
            VMEM(slot_blocks.shape, jnp.int32),
            SMEM(slot_counts.shape, jnp.int32),
            SMEM(quad_weights.shape, F32),
            VMEM((4, tiles, LANES), F32),
            pltpu.SemaphoreType.DMA((8,)),
        ],
        compiler_params=params(24),
        name="pack",
    )
    operands = (
        stay(slot_counts),
        stay(quad_weights),
        stay(edge_basis.T),
        stay(forward_edges.transpose(1, 0, 2)),
        stay(adjoint_edges.transpose(1, 0, 2)),
        stay(slot_weights),
        stay(slot_elements),
        stay(slot_blocks),
    )
    payload = call(*operands)

    arrived = lax.all_to_all(payload, ("tx", "ty"), split_axis=0, concat_axis=0, tiled=True)
    strip = shape((NEAR, inner, LANES), BF16)
    rim_edge = shape((RADIUS * edge_rows, LANES), BF16)
    call = pl.pallas_call(
        cast_kernel,
        out_shape=(rim_edge,) * 2 + (strip,) * 4,
        in_specs=[anywhere] * 2,
        out_specs=(whole,) * 6,
        scratch_shapes=[
            VMEM((2 * RADIUS, cells_y, cells_z), F32),
            pltpu.SemaphoreType.DMA((2,)),
        ],
        compiler_params=params(16),
        name="cast_rims",
    )
    up_first, down_first, *mains = call(stay(design), stay(payload))
    low_first = lax.ppermute(up_first, "tx", up)
    high_first = lax.ppermute(down_first, "tx", down)

    call = pl.pallas_call(
        prefix_kernel,
        out_shape=shape((LANES, LANES), BF16),
        in_specs=[anywhere],
        out_specs=whole,
        compiler_params=params(16),
        name="prefix",
    )
    prefix = call(up_first)
    low_near = lax.ppermute(mains[0], "tx", up)
    high_near = lax.ppermute(mains[1], "tx", down)
    low_far = lax.ppermute(mains[2], "tx", up)
    high_far = lax.ppermute(mains[3], "tx", down)

    grid, edge_smooth, small, rim, rows_own = pl.pallas_call(
        functools.partial(deposit_kernel, cells_y, slots),
        out_shape=(
            shape((rows_ext, cells_z), F32),
            shape((cells_x, 2 * RADIUS, cells_z), F32),
            shape((cells_x, LANES), BF16),
            shape((cells_x, RADIUS, cells_y), BF16),
            shape((tiles, LANES), jnp.int32),
        ),
        in_specs=[anywhere] + [whole] * 4,
        out_specs=(whole,) * 5,
        scratch_shapes=[
            VMEM((cells_x + 2 * RADIUS, RADIUS, cells_y), F32),
            VMEM((tiles * slots, LANES), F32),
            VMEM((tiles, LANES), jnp.int32),
            VMEM((tiles, LANES), F32),
            SMEM((tiles, LANES), jnp.int32),
            SMEM((tiles, LANES), F32),
            pltpu.SemaphoreType.DMA((5,)),
        ],
        compiler_params=params(16),
        name="deposit",
    )(stay(design.reshape(cells_x * cells_y, cells_z)), low_first, high_first, arrived, prefix)

    small = lax.ppermute(small, "gz", [(0, 1), (1, 0)])
    rim = lax.ppermute(rim, "gz", [(0, 1), (1, 0)])
    edge = shape((cells_x, RADIUS, cells_z), BF16)
    call = pl.pallas_call(
        edge_kernel,
        out_shape=(edge, edge),
        in_specs=[whole, whole],
        out_specs=(whole, whole),
        compiler_params=params(16),
        name="edges",
    )
    first, last = call(edge_smooth, small)
    up = [(i, (i + 1) % n_ty) for i in range(n_ty)]
    down = [(t, s) for s, t in up]
    before = lax.ppermute(last, "ty", up)
    after = lax.ppermute(first, "ty", down)

    flat = shape((cells_x * cells_y, cells_z), F32)
    constants = (float(TAPS**4), n_gz * cells_z)
    call = pl.pallas_call(
        functools.partial(inner_kernel, *constants),
        out_shape=(flat, shape((2, cells_x * RADIUS, cells_z), F32)),
        in_specs=[whole] * 6,
        out_specs=(whole, whole),
        scratch_shapes=[
            VMEM((2 * RADIUS, cells_y, cells_z), BF16),
            VMEM((cells_x - RADIUS, cells_y, cells_z), BF16),
        ],
        compiler_params=params(16),
        name="inner",
    )
    partial, ends = call(grid, low_near, high_near, rim, before, after)
    _, projected, ratios = pl.pallas_call(
        functools.partial(finish_kernel, *constants),
        out_shape=(flat, flat, shape((tiles * capacity // LANES, LANES), F32)),
        in_specs=[whole] * 10,
        out_specs=(whole, anywhere, whole),
        scratch_shapes=[
            VMEM((2 * RADIUS, cells_y, cells_z), BF16),
            VMEM((RADIUS, cells_y, cells_z), BF16),
            VMEM((tiles * capacity, cells_z), F32),
            SMEM((tiles, LANES), jnp.int32),
            pltpu.SemaphoreType.DMA((3,)),
            pltpu.SemaphoreType.DMA,
        ],
        input_output_aliases={0: 0},
        compiler_params=params(16),
        name="finish",
    )(
        partial, rows_own, grid, low_near, high_near, low_far, high_far, rim, ends, arrived
    )

    ratios = ratios.reshape(tiles, capacity)
    ratios = lax.all_to_all(ratios, ("tx", "ty"), split_axis=0, concat_axis=0, tiled=True)
    density = pl.pallas_call(
        back_kernel,
        out_shape=shape((elements // LANES, LANES), F32),
        in_specs=[whole] * 3,
        out_specs=whole,
        compiler_params=params(16),
        name="to_elements",
    )(slot_counts, slot_elements, ratios)
    return projected.reshape(design.shape), density.reshape(elements)


def solution(mesh):
    in_specs = (
        P("tx", "ty", "gz"),
        P(None, None, ("tx", "ty", "gz")),
        P(None, None, ("tx", "ty", "gz")),
        P(),
        P(),
        P(("tx", "ty", "gz"), None, None),
        P(("tx", "ty", "gz"), None),
        P(("tx", "ty", "gz"), None),
        P(("tx", "ty", "gz"), None),
    )
    out_specs = (P("tx", "ty", "gz"), P(("tx", "ty", "gz")))
    return jax.shard_map(update, mesh=mesh, in_specs=in_specs, out_specs=out_specs, check_vma=False)
```

```python
import functools
import math

import jax
import jax.numpy as jnp
from jax import lax
from jax.experimental import pallas as pl
from jax.experimental.pallas import tpu as pltpu
from jax.sharding import PartitionSpec as P


RADIUS = 8
LANES = 128
TAPS = RADIUS + 1
STEP = 8
NEAR = RADIUS // 2
GROUP = 6
F32 = jnp.float32
BF16 = jnp.bfloat16
SMEM = pltpu.SMEM
VMEM = pltpu.VMEM
NT = ((1,), (1,))


def iota(shape, dim):
    return lax.broadcasted_iota(jnp.int32, shape, dim)


def onehot(mask):
    return mask.astype(F32).astype(BF16)


def cone(distance):
    return jnp.maximum(TAPS - jnp.abs(distance), 0).astype(F32).astype(BF16)


def halves(x):
    high = x.astype(BF16)
    return high, (x - high.astype(F32)).astype(BF16)


def dot(a, b, contract=((1,), (0,)), precision=None):
    return lax.dot_general(
        a, b, (contract, ((), ())), preferred_element_type=F32, precision=precision
    )


def picker():
    first = jnp.where(lax.axis_index("gz") == 0, LANES - RADIUS, 0)
    return onehot(iota((RADIUS, LANES), 1) == iota((RADIUS, LANES), 0) + first)


def side_weights():
    first = jnp.where(lax.axis_index("gz") == 0, LANES, -RADIUS)
    return cone(iota((RADIUS, LANES), 0) + first - iota((RADIUS, LANES), 1))


def running(planes, length):
    add = lambda a, b: a + b
    box = [functools.reduce(add, planes[:TAPS])]
    for k in range(length + RADIUS - 1):
        box.append(box[-1] + (planes[k + TAPS] - planes[k]))
    total = functools.reduce(add, box[:TAPS])
    out = [total]
    for i in range(length - 1):
        total = total + (box[i + TAPS] - box[i])
        out.append(total)
    return out


def clipped(x):
    return jnp.clip(x, -0.5, 0.5)


def pack_kernel(
    n_ty, cells_x, cells_y, counts_hbm, quad_hbm, basis_hbm, forward_hbm, adjoint_hbm, weights_hbm,
    elements_hbm, blocks_hbm, pay_ref, basis_ref, forward_ref, adjoint_ref, weights_ref,
    elements_ref, blocks_ref, counts_ref, quad_ref, code_ref, sem,
):
    sources = (forward_hbm, adjoint_hbm, basis_hbm, elements_hbm, blocks_hbm, weights_hbm)
    sources += (counts_hbm, quad_hbm)
    targets = (forward_ref, adjoint_ref, basis_ref, elements_ref, blocks_ref, weights_ref)
    targets += (counts_ref, quad_ref)
    loads = [
        pltpu.make_async_copy(source, target, sem.at[i])
        for i, (source, target) in enumerate(zip(sources, targets))
    ]
    for load in loads:
        load.start()
    tiles, capacity = elements_ref.shape
    points = quad_ref.shape[0]
    highest = lax.Precision.HIGHEST
    for load in loads:
        load.wait()

    terms, edges = 2 * forward_ref.shape[0], forward_ref.shape[0]
    point = iota((1, 3 * points), 1) % points
    quad = jnp.zeros((1, 3 * points), F32)
    for q in range(points):
        quad = quad + jnp.where(point == q, quad_ref[q], 0.0)
    twice = (iota((terms, edges), 0) // 2 == iota((terms, edges), 1)).astype(F32)
    basis = dot(twice, basis_ref[...], precision=highest)
    gram = dot(basis * quad, basis, NT, precision=highest)
    row, column = iota((terms, terms), 0), iota((terms, terms), 1)
    gram = jnp.where(row % 2 == 0, gram, -gram)
    gram = jnp.where(row % 2 == column % 2, gram, 0.0)
    adjoint = jnp.concatenate([adjoint_ref[k] for k in range(edges)], axis=0)
    forward = jnp.concatenate([forward_ref[k] for k in range(edges)], axis=0)
    (gram_a, gram_b), (field_a, field_b) = halves(gram), halves(adjoint)
    left = [gram_a.astype(F32), gram_b.astype(F32), gram_a.astype(F32)]
    right = [field_a.astype(F32), field_a.astype(F32), field_b.astype(F32)]
    left = jnp.concatenate(left, axis=1).astype(BF16)
    mixed = dot(left, jnp.concatenate(right, axis=0).astype(BF16))
    sens = jnp.sum(forward * mixed, axis=0, keepdims=True)
    groups = sens.shape[1] // LANES
    sens = jnp.concatenate([sens[:, g * LANES : (g + 1) * LANES] for g in range(groups)], axis=0)
    first, _ = halves(sens)
    second, third = halves(sens - first.astype(F32))
    parts = jnp.concatenate([first, second, third], axis=0)

    element, block = elements_ref[...], blocks_ref[...]
    codes = [
        element // LANES,
        element % LANES,
        block // cells_y + RADIUS,
        block % cells_y,
    ]
    place = iota((capacity, LANES), 1) - iota((capacity, LANES), 0)
    for index, code in enumerate(codes):
        code = code.astype(F32).astype(BF16)
        total = jnp.zeros((tiles, LANES), F32)
        for order, d in enumerate((0, -1, 1)):
            moved = dot(code, onehot(place == order * capacity))
            shift = (d * n_ty) % tiles
            if shift:
                moved = jnp.concatenate([moved[shift:], moved[:shift]], axis=0)
            if index == 2 and d:
                group = iota((tiles, LANES), 1) // capacity
                moved = moved + jnp.where(group == order, float(d * cells_x), 0.0)
            total = total + moved
        code_ref[index] = total

    @pl.loop(0, tiles, unroll=min(tiles, 16))
    def _(t):
        high, low, plane, line = (code_ref[index, pl.ds(t, 1), :] for index in range(4))
        lane = iota((1, LANES), 1)
        live = jnp.zeros((1, LANES), jnp.bool_)
        sources = []
        for order, d in enumerate((0, -1, 1)):
            source = lax.rem(t + (d * n_ty) % tiles, tiles)
            sources.append(source)
            at = lane - order * capacity
            live = live | ((at >= 0) & (at < capacity) & (at < counts_ref[0, source]))
        hit = onehot(iota((LANES, LANES), 0).astype(F32) == low)
        found = dot(parts, hit)
        found = (found[:groups] + found[groups : 2 * groups]) + found[2 * groups :]
        mine = iota((groups, LANES), 0).astype(F32) == high
        value = jnp.sum(jnp.where(mine, found, 0.0), axis=0, keepdims=True)
        value = jnp.where(live, value, 0.0).astype(BF16).astype(F32) * -0.5
        kind = iota((8, LANES), 0)
        meta = jnp.where(kind == 0, plane, jnp.where(kind == 1, line, value))
        meta = jnp.where(kind < 3, meta, 0.0)
        for order, source in enumerate(sources):
            pay_ref[t, order * capacity : (order + 1) * capacity, :] = weights_ref[source]
        pay_ref[t, 3 * capacity :, :] = meta.astype(BF16)


def strips(design_ref, strip_ref, sem):
    cells_x = design_ref.shape[0]
    return [
        pltpu.make_async_copy(
            design_ref.at[pl.ds(start, RADIUS)], strip_ref.at[pl.ds(side * RADIUS, RADIUS)],
            sem.at[side],
        )
        for side, start in enumerate((0, cells_x - RADIUS))
    ]


def cast_kernel(
    design_ref, token_ref, up_ref, down_ref, up_near_ref, down_near_ref, up_far_ref, down_far_ref,
    strip_ref, sem,
):
    cells_y = design_ref.shape[1]
    edge_rows = 2 * RADIUS + RADIUS * cells_y // LANES
    copies = strips(design_ref, strip_ref, sem)
    for copy in copies:
        copy.start()
    pick = picker()
    by_side = ((down_ref, down_near_ref, down_far_ref), (up_ref, up_far_ref, up_near_ref))
    for side, targets in enumerate(by_side):
        copies[side].wait()
        for p in range(RADIUS):
            plane = strip_ref[side * RADIUS + p] - 0.5
            targets[1 + p // NEAR][p % NEAR] = plane[RADIUS : cells_y - RADIUS].astype(BF16)
            flipped = dot(pick, plane.astype(BF16), NT)
            pieces = [plane[:RADIUS], plane[cells_y - RADIUS :]]
            pieces += [flipped[:, k * LANES : (k + 1) * LANES] for k in range(cells_y // LANES)]
            pieces = jnp.concatenate(pieces, axis=0).astype(BF16)
            targets[0][p * edge_rows : (p + 1) * edge_rows, :] = pieces


def prefix_kernel(token_ref, out_ref):
    out_ref[...] = onehot(iota((LANES, LANES), 0) <= iota((LANES, LANES), 1))


def deposit_kernel(
    cells_y, slots, design_ref, low_ref, high_ref, pay_ref, prefix_ref, grid_ref, rows_out_ref,
    small_ref, rim_ref, own_ref, flip_ref, weight_ref, code_ref, value_ref, code_smem, value_smem, sem,
):
    cells_x = design_ref.shape[0] // cells_y
    partners = pay_ref.shape[0]
    rim = RADIUS * cells_y
    own = cells_x * cells_y
    edge_rows = 2 * RADIUS + RADIUS * cells_y // LANES
    copy = pltpu.make_async_copy(design_ref, grid_ref.at[pl.ds(rim, own)], sem.at[0])
    copy.start()

    lane = iota((1, LANES), 1)
    upper = prefix_ref[...]

    def decode(p):
        weight_ref[pl.ds(pl.multiple_of(p * slots, 16), slots), :] = pay_ref[p, :slots, :].astype(F32)
        meta = pay_ref[p, slots : slots + 8, :].astype(F32)
        plane, line, value = meta[0:1], meta[1:2], meta[2:3]
        own_ref[pl.ds(p, 1), :] = ((plane - float(RADIUS)) * float(cells_y) + line).astype(jnp.int32)
        used = (plane >= 0.0) & (plane < float(cells_x + 2 * RADIUS)) & (value != 0.0)
        used = jnp.where(used & (lane < slots), 1.0, 0.0)
        order = dot(jnp.broadcast_to(used, (8, LANES)).astype(BF16), upper)[:1]
        place = jnp.where(used > 0.0, order - 1.0, -1.0)
        hit = onehot(iota((LANES, LANES), 0).astype(F32) == place)
        kind = iota((8, LANES), 0)
        meta = jnp.where(kind == 3, lane.astype(F32), jnp.where(kind < 3, meta, 0.0))
        moved = dot(meta.astype(BF16), hit, NT)
        code = (moved[0:1] * float(cells_y) + moved[1:2]) * float(LANES) + moved[3:4]
        code = jnp.where(lane == LANES - 1, order[:, LANES - 1 :], code)
        code_ref[pl.ds(p, 1), :] = code.astype(jnp.int32)
        value_ref[pl.ds(p, 1), :] = moved[2:3]

    half = partners // 2
    lists = []
    for h in range(2):
        part = pl.ds(h * half, half)
        pl.loop(h * half, (h + 1) * half, unroll=min(half, 8))(decode)
        moves = [
            pltpu.make_async_copy(code_ref.at[part], code_smem.at[part], sem.at[1 + 2 * h]),
            pltpu.make_async_copy(value_ref.at[part], value_smem.at[part], sem.at[2 + 2 * h]),
        ]
        for move in moves:
            move.start()
        lists.append(moves)
    zeros = jnp.zeros((cells_y, LANES), F32)
    for p in range(RADIUS):
        grid_ref[p * cells_y : (p + 1) * cells_y, :] = zeros
        grid_ref[rim + own + p * cells_y : rim + own + (p + 1) * cells_y, :] = zeros
    copy.wait()

    def scatter(p):
        @pl.loop(0, (code_smem[p, LANES - 1] + GROUP - 1) // GROUP)
        def _(j):
            codes = [code_smem[p, j * GROUP + k] for k in range(GROUP)]
            spots = [code // LANES for code in codes]
            amounts = [
                value_smem[p, j * GROUP + k] * weight_ref[pl.ds(p * slots + codes[k] % LANES, 1), :]
                for k in range(GROUP)
            ]
            olds = [grid_ref[pl.ds(spot, 1), :] for spot in spots]
            for k in range(GROUP):
                amount = amounts[k]
                for i in range(k):
                    amount = amount + jnp.where(spots[i] == spots[k], 1.0, 0.0) * amounts[i]
                grid_ref[pl.ds(spots[k], 1), :] = olds[k] + amount

    for h in range(2):
        for move in lists[h]:
            move.wait()
        pl.loop(h * half, (h + 1) * half)(scatter)

    total = cells_x + 2 * RADIUS
    pick = picker()

    @pl.loop(0, cells_x, unroll=16)
    def _(x):
        plane = clipped(grid_ref[pl.ds(rim + x * cells_y, cells_y), :] - 0.5)
        flip_ref[x + RADIUS] = dot(pick, plane.astype(BF16), NT)

    for source_ref, base in ((low_ref, 0), (high_ref, RADIUS + cells_x)):
        for p in range(RADIUS):
            plane = grid_ref[pl.ds((base + p) * cells_y, cells_y), :]
            deposited = dot(pick, plane.astype(BF16), NT)
            raw = jnp.concatenate(
                [
                    source_ref[pl.ds(p * edge_rows + (2 + k) * RADIUS, RADIUS), :].astype(F32)
                    for k in range(cells_y // LANES)
                ],
                axis=1,
            )
            flip_ref[base + p] = clipped(raw + deposited)

    for source_ref, base in ((low_ref, 0), (high_ref, RADIUS + cells_x)):
        for p in range(RADIUS):
            for k, start in enumerate((0, cells_y - RADIUS)):
                at = (base + p) * cells_y + start
                edge = source_ref[p * edge_rows + k * RADIUS : p * edge_rows + (k + 1) * RADIUS, :]
                edge = edge.astype(F32)
                grid_ref[at : at + RADIUS, :] = grid_ref[at : at + RADIUS, :] + edge

    for k, start in enumerate((0, cells_y - RADIUS)):
        planes = []
        for e in range(total):
            at = e * cells_y + start
            bias = 0.5 if RADIUS <= e < RADIUS + cells_x else 0.0
            planes.append(clipped(grid_ref[at : at + RADIUS, :] - bias))
        for i, value in enumerate(running(planes, cells_x)):
            rows_out_ref[i, k * RADIUS : (k + 1) * RADIUS, :] = value

    double = 2 * RADIUS
    rows = rows_out_ref[...].reshape(cells_x * double, LANES).astype(BF16)
    first = jnp.where(lax.axis_index("gz") == 0, LANES - RADIUS, 0)
    tiled = onehot(iota((LANES, LANES), 0) == iota((LANES, LANES), 1) % RADIUS + first)
    shape = (cells_x * double, LANES)
    mine = iota(shape, 0) % double == iota(shape, 1) // RADIUS
    small = jnp.where(mine, dot(rows, tiled), 0.0).reshape(cells_x, double, LANES)
    small_ref[...] = jnp.sum(small, axis=1).astype(BF16)

    for i, value in enumerate(running([flip_ref[e] for e in range(total)], cells_x)):
        rim_ref[i] = value.astype(BF16)


def edge_kernel(rows_ref, small_ref, first_ref, last_ref):
    cells_x, double, cells_z = rows_ref.shape
    weights = cone(iota((cells_z, cells_z), 0) - iota((cells_z, cells_z), 1))
    weights = jnp.concatenate([weights, weights], axis=0)
    side = jnp.concatenate([side_weights()] * double, axis=0)
    rows = rows_ref[...].reshape(cells_x * double, cells_z)
    shape = (cells_x * double, LANES)
    repeat = onehot(iota((shape[0], cells_x), 0) // double == iota((shape[0], cells_x), 1))
    mine = iota(shape, 0) % double == iota(shape, 1) // RADIUS
    spread = jnp.where(mine, dot(repeat, small_ref[...]), 0.0).astype(BF16)
    value = dot(jnp.concatenate(halves(rows), axis=1), weights) + dot(spread, side)
    value = value.astype(BF16)
    for x in range(cells_x):
        first_ref[x] = value[x * double : x * double + RADIUS]
        last_ref[x] = value[x * double + RADIUS : (x + 1) * double]


def project_planes(
    scale_total, depth, places, step, smooth_ref, rim_ref, ends_ref, proj_ref, done
):
    _, _, cells_y = rim_ref.shape
    cells_z = proj_ref.shape[1]
    across = cone(iota((cells_y, cells_y), 0) - iota((cells_y, cells_y), 1))
    along = cone(iota((cells_z, cells_z), 0) - iota((cells_z, cells_z), 1))
    along = jnp.concatenate([along, side_weights()], axis=0)
    z = iota((1, cells_z), 1) + lax.axis_index("gz") * cells_z
    inside = jnp.zeros((1, cells_z), F32)
    for offset in range(-RADIUS, RADIUS + 1):
        good = (z + offset >= 0) & (z + offset < depth)
        inside = inside + jnp.where(good, float(TAPS - abs(offset)), 0.0)
    scale = 8.0 / (scale_total * inside)
    top = math.tanh(4.0)

    @pl.loop(0, places[1], unroll=STEP // step)
    def _(g):
        base = places[0] + g * places[2]
        rims = rim_ref[pl.ds(base, step)].reshape(step * RADIUS, cells_y)
        rims = dot(rims, across)
        for pair in range(step // 2):
            both = [smooth_ref[g * step + 2 * pair + k] for k in range(2)]
            both = dot(across, jnp.concatenate(both, axis=1)).astype(BF16)
            for k in range(2):
                x = base + 2 * pair + k
                at = (2 * pair + k) * RADIUS
                flipped = rims[at : at + RADIUS].T.astype(BF16)
                half = both[:, k * cells_z : (k + 1) * cells_z]
                value = dot(jnp.concatenate([half, flipped], axis=1), along)
                spot = pl.ds(pl.multiple_of(x * RADIUS, RADIUS), RADIUS)
                first = value[:RADIUS] + ends_ref[0, spot, :]
                last = value[cells_y - RADIUS :] + ends_ref[1, spot, :]
                value = jnp.concatenate([first, value[RADIUS : cells_y - RADIUS], last], axis=0)
                value = (top + jnp.tanh(value * scale)) * (1.0 / (2.0 * top))
                proj_ref[pl.ds(pl.multiple_of(x * cells_y, 8), cells_y), :] = value
        done(g)


def smooth_x(grid_ref, pad_ref, low, high, start, rows, main):
    cells_y = pad_ref.shape[1]
    cells_x = grid_ref.shape[0] // cells_y - 2 * RADIUS

    def plane(e):
        at = pl.multiple_of(e * cells_y + start, rows)
        value = grid_ref[pl.ds(at, rows), :]
        if RADIUS <= e < RADIUS + cells_x:
            return clipped(value - 0.5)
        p = e if e < RADIUS else e - cells_x
        rim = pad_ref[p, pl.ds(start, rows), :].astype(F32)
        return clipped(value + jnp.where(main, rim, 0.0))

    return running([plane(e) for e in range(low, high + 2 * RADIUS)], high - low)


def main_rows(start, rows, cells_y):
    row = start + iota((rows, 1), 0)
    return (row >= RADIUS) & (row < cells_y - RADIUS)


def inner_kernel(
    scale_total, depth, grid_ref, low_ref, high_ref, rim_ref, before_ref, after_ref, proj_ref,
    ends_ref, pad_ref, smooth_ref,
):
    cells_x, _, cells_y = rim_ref.shape
    cells_z = proj_ref.shape[1]
    many = cells_x * RADIUS
    row, column = iota((many, many), 0), iota((many, many), 1)
    same = row // RADIUS == column // RADIUS
    gap = row % RADIUS - column % RADIUS
    for rows_in_ref, distance, index in ((before_ref, gap + RADIUS, 0), (after_ref, gap - RADIUS, 1)):
        weights = jnp.where(same, cone(distance).astype(F32), 0.0).astype(BF16)
        ends_ref[index] = dot(weights, rows_in_ref[...].reshape(many, cells_z))
    count = cells_x - RADIUS
    chunk = 16
    for p in range(NEAR):
        pad_ref[NEAR + p, RADIUS : cells_y - RADIUS, :] = low_ref[p]
        pad_ref[RADIUS + p, RADIUS : cells_y - RADIUS, :] = high_ref[p]

    @pl.loop(0, cells_y // chunk)
    def _(j):
        start = pl.multiple_of(j * chunk, chunk)
        main = main_rows(start, chunk, cells_y)
        values = smooth_x(grid_ref, pad_ref, NEAR, cells_x - NEAR, start, chunk, main)
        for i, value in enumerate(values):
            smooth_ref[i, pl.ds(start, chunk), :] = value.astype(BF16)

    project_planes(
        scale_total, depth, (NEAR, count // STEP, STEP), STEP, smooth_ref, rim_ref, ends_ref,
        proj_ref, lambda g: None,
    )


def finish_kernel(
    scale_total, depth, inner_ref, own_ref, grid_ref, low_near_ref, high_near_ref, low_far_ref,
    high_far_ref, rim_ref, ends_ref, pay_ref, proj_ref, out_ref, ratio_ref, pad_ref, smooth_ref,
    picked_ref, rows_ref, sem, own_sem,
):
    cells_x, _, cells_y = rim_ref.shape
    cells_z = out_ref.shape[1]
    partners = pay_ref.shape[0]
    capacity = picked_ref.shape[0] // partners
    chunk = 16
    fetch = pltpu.make_async_copy(own_ref, rows_ref, own_sem)
    fetch.start()

    def send(first, count, index):
        rows = pl.ds(pl.multiple_of(first * cells_y, 8), count * cells_y)
        return pltpu.make_async_copy(proj_ref.at[rows], out_ref.at[rows], sem.at[index])

    inner_send = send(NEAR, cells_x - RADIUS, 2)
    inner_send.start()
    sources = (low_far_ref, low_near_ref, high_near_ref, high_far_ref)
    for index, source_ref in enumerate(sources):
        for p in range(NEAR):
            pad_ref[index * NEAR + p, RADIUS : cells_y - RADIUS, :] = source_ref[p]

    @pl.loop(0, cells_y // chunk)
    def _(j):
        start = pl.multiple_of(j * chunk, chunk)
        main = main_rows(start, chunk, cells_y)
        values = smooth_x(grid_ref, pad_ref, 0, NEAR, start, chunk, main)
        values += smooth_x(grid_ref, pad_ref, cells_x - NEAR, cells_x, start, chunk, main)
        for i, value in enumerate(values):
            smooth_ref[i, pl.ds(start, chunk), :] = value.astype(BF16)

    last = cells_x - NEAR
    project_planes(
        scale_total, depth, (0, 2, last), NEAR, smooth_ref, rim_ref, ends_ref, proj_ref,
        lambda g: send(g * last, NEAR, g).start(),
    )
    fetch.wait()

    @pl.loop(0, partners)
    def _(p):
        for s in range(capacity):
            row = rows_ref[p, s]
            picked_ref[pl.ds(p * capacity + s, 1), :] = proj_ref[pl.ds(row, 1), :]

    ones = jnp.ones((8, cells_z), BF16)
    group = LANES // capacity

    @pl.loop(0, partners * capacity // LANES)
    def _(c):
        w = pay_ref[pl.ds(c * group, group), :capacity, :].reshape(LANES, cells_z)
        picked = picked_ref[pl.ds(pl.multiple_of(c * LANES, LANES), LANES), :]
        high, low = halves(w.astype(F32) * picked)
        amount = dot(ones, high, NT) + dot(ones, low, NT)
        ratio_ref[pl.ds(c, 1), :] = (amount / dot(ones, w, NT))[:1]

    for g in range(2):
        send(g * last, NEAR, g).wait()
    inner_send.wait()


def back_kernel(counts_ref, elements_ref, ratio_ref, out_ref):
    tiles, capacity = elements_ref.shape
    high_count = out_ref.shape[0]
    group = min(tiles, 16)
    wide = group * capacity
    out_ref[...] = jnp.zeros(out_ref.shape, F32)

    @pl.loop(0, tiles // group)
    def _(g):
        start = pl.multiple_of(g * group, group)
        element = elements_ref[pl.ds(start, group), :]
        tile = iota((group, tiles), 0) + start == iota((group, tiles), 1)
        counts = jnp.where(tile, counts_ref[...].astype(F32), 0.0)
        counts = jnp.sum(counts, axis=1, keepdims=True)
        live = iota((group, capacity), 1).astype(F32) < counts
        ratio = jnp.where(live, ratio_ref[pl.ds(start, group), :], 0.0)
        first, _ = halves(ratio)
        second, third = halves(ratio - first.astype(F32))
        parts = [(element // LANES).astype(F32), (element % LANES).astype(F32)]
        parts += [part.astype(F32) for part in (first, second, third)]
        spread = onehot(iota((capacity, wide), 1) % capacity == iota((capacity, wide), 0))
        own = iota((group, wide), 1) // capacity == iota((group, wide), 0)
        rows = []
        for part in parts:
            part = jnp.where(own, dot(part.astype(BF16), spread), 0.0)
            rows.append(jnp.sum(part, axis=0, keepdims=True))
        lane = onehot(iota((LANES, wide), 0).astype(F32) == rows[1])
        mine = iota((high_count, wide), 0).astype(F32) == rows[0]
        total = jnp.zeros(out_ref.shape, F32)
        for part in rows[2:]:
            total = total + dot(jnp.where(mine, part, 0.0).astype(BF16), lane, NT)
        out_ref[...] = out_ref[...] + total


def update(
    design,
    forward_edges,
    adjoint_edges,
    edge_basis,
    quad_weights,
    slot_weights,
    slot_elements,
    slot_blocks,
    slot_counts,
):
    cells_x, cells_y, cells_z = design.shape
    tiles, capacity = slot_elements.shape
    n_tx, n_ty, n_gz = (lax.axis_size(a) for a in ("tx", "ty", "gz"))
    if cells_z != LANES or cells_y != 256 or n_gz != 2:
        raise NotImplementedError
    slots = 3 * capacity
    edge_count, elements = forward_edges.shape[1:]
    rows_ext = (cells_x + 2 * RADIUS) * cells_y
    whole = pl.BlockSpec(memory_space=VMEM)
    anywhere = pl.BlockSpec(memory_space=pltpu.HBM)
    shape = jax.ShapeDtypeStruct
    stay = lambda x: pltpu.with_memory_space_constraint(x, pltpu.HBM)
    params = lambda mib: pltpu.CompilerParams(vmem_limit_bytes=mib << 20)

    inner = cells_y - 2 * RADIUS
    edge_rows = 2 * RADIUS + RADIUS * cells_y // LANES
    up = [(i, (i + 1) % n_tx) for i in range(n_tx)]
    down = [(t, s) for s, t in up]

    call = pl.pallas_call(
        functools.partial(pack_kernel, n_ty, cells_x, cells_y),
        out_shape=shape((tiles, slots + 8, LANES), BF16),
        in_specs=[anywhere] * 8,
        out_specs=whole,
        scratch_shapes=[
            VMEM(edge_basis.shape[::-1], F32),
            VMEM((edge_count, 2, elements), F32),
            VMEM((edge_count, 2, elements), F32),
            VMEM(slot_weights.shape, BF16),
            VMEM(slot_elements.shape, jnp.int32),
            VMEM(slot_blocks.shape, jnp.int32),
            SMEM(slot_counts.shape, jnp.int32),
            SMEM(quad_weights.shape, F32),
            VMEM((4, tiles, LANES), F32),
            pltpu.SemaphoreType.DMA((8,)),
        ],
        compiler_params=params(24),
        name="pack",
    )
    operands = (
        stay(slot_counts),
        stay(quad_weights),
        stay(edge_basis.T),
        stay(forward_edges.transpose(1, 0, 2)),
        stay(adjoint_edges.transpose(1, 0, 2)),
        stay(slot_weights),
        stay(slot_elements),
        stay(slot_blocks),
    )
    payload = call(*operands)

    arrived = lax.all_to_all(payload, ("tx", "ty"), split_axis=0, concat_axis=0, tiled=True)
    strip = shape((NEAR, inner, LANES), BF16)
    rim_edge = shape((RADIUS * edge_rows, LANES), BF16)
    call = pl.pallas_call(
        cast_kernel,
        out_shape=(rim_edge,) * 2 + (strip,) * 4,
        in_specs=[anywhere] * 2,
        out_specs=(whole,) * 6,
        scratch_shapes=[
            VMEM((2 * RADIUS, cells_y, cells_z), F32),
            pltpu.SemaphoreType.DMA((2,)),
        ],
        compiler_params=params(16),
        name="cast_rims",
    )
    up_first, down_first, *mains = call(stay(design), stay(payload))
    low_first = lax.ppermute(up_first, "tx", up)
    high_first = lax.ppermute(down_first, "tx", down)

    call = pl.pallas_call(
        prefix_kernel,
        out_shape=shape((LANES, LANES), BF16),
        in_specs=[anywhere],
        out_specs=whole,
        compiler_params=params(16),
        name="prefix",
    )
    prefix = call(up_first)
    low_near = lax.ppermute(mains[0], "tx", up)
    high_near = lax.ppermute(mains[1], "tx", down)
    low_far = lax.ppermute(mains[2], "tx", up)
    high_far = lax.ppermute(mains[3], "tx", down)

    grid, edge_smooth, small, rim, rows_own = pl.pallas_call(
        functools.partial(deposit_kernel, cells_y, slots),
        out_shape=(
            shape((rows_ext, cells_z), F32),
            shape((cells_x, 2 * RADIUS, cells_z), F32),
            shape((cells_x, LANES), BF16),
            shape((cells_x, RADIUS, cells_y), BF16),
            shape((tiles, LANES), jnp.int32),
        ),
        in_specs=[anywhere] + [whole] * 4,
        out_specs=(whole,) * 5,
        scratch_shapes=[
            VMEM((cells_x + 2 * RADIUS, RADIUS, cells_y), F32),
            VMEM((tiles * slots, LANES), F32),
            VMEM((tiles, LANES), jnp.int32),
            VMEM((tiles, LANES), F32),
            SMEM((tiles, LANES), jnp.int32),
            SMEM((tiles, LANES), F32),
            pltpu.SemaphoreType.DMA((5,)),
        ],
        compiler_params=params(16),
        name="deposit",
    )(stay(design.reshape(cells_x * cells_y, cells_z)), low_first, high_first, arrived, prefix)

    small = lax.ppermute(small, "gz", [(0, 1), (1, 0)])
    rim = lax.ppermute(rim, "gz", [(0, 1), (1, 0)])
    edge = shape((cells_x, RADIUS, cells_z), BF16)
    call = pl.pallas_call(
        edge_kernel,
        out_shape=(edge, edge),
        in_specs=[whole, whole],
        out_specs=(whole, whole),
        compiler_params=params(16),
        name="edges",
    )
    first, last = call(edge_smooth, small)
    up = [(i, (i + 1) % n_ty) for i in range(n_ty)]
    down = [(t, s) for s, t in up]
    before = lax.ppermute(last, "ty", up)
    after = lax.ppermute(first, "ty", down)

    flat = shape((cells_x * cells_y, cells_z), F32)
    constants = (float(TAPS**4), n_gz * cells_z)
    call = pl.pallas_call(
        functools.partial(inner_kernel, *constants),
        out_shape=(flat, shape((2, cells_x * RADIUS, cells_z), F32)),
        in_specs=[whole] * 6,
        out_specs=(whole, whole),
        scratch_shapes=[
            VMEM((2 * RADIUS, cells_y, cells_z), BF16),
            VMEM((cells_x - RADIUS, cells_y, cells_z), BF16),
        ],
        compiler_params=params(16),
        name="inner",
    )
    partial, ends = call(grid, low_near, high_near, rim, before, after)
    _, projected, ratios = pl.pallas_call(
        functools.partial(finish_kernel, *constants),
        out_shape=(flat, flat, shape((tiles * capacity // LANES, LANES), F32)),
        in_specs=[whole] * 10,
        out_specs=(whole, anywhere, whole),
        scratch_shapes=[
            VMEM((2 * RADIUS, cells_y, cells_z), BF16),
            VMEM((RADIUS, cells_y, cells_z), BF16),
            VMEM((tiles * capacity, cells_z), F32),
            SMEM((tiles, LANES), jnp.int32),
            pltpu.SemaphoreType.DMA((3,)),
            pltpu.SemaphoreType.DMA,
        ],
        input_output_aliases={0: 0},
        compiler_params=params(16),
        name="finish",
    )(
        partial, rows_own, grid, low_near, high_near, low_far, high_far, rim, ends, arrived
    )

    ratios = ratios.reshape(tiles, capacity)
    ratios = lax.all_to_all(ratios, ("tx", "ty"), split_axis=0, concat_axis=0, tiled=True)
    density = pl.pallas_call(
        back_kernel,
        out_shape=shape((elements // LANES, LANES), F32),
        in_specs=[whole] * 3,
        out_specs=whole,
        compiler_params=params(16),
        name="to_elements",
    )(slot_counts, slot_elements, ratios)
    return projected.reshape(design.shape), density.reshape(elements)


def solution(mesh):
    in_specs = (
        P("tx", "ty", "gz"),
        P(None, None, ("tx", "ty", "gz")),
        P(None, None, ("tx", "ty", "gz")),
        P(),
        P(),
        P(("tx", "ty", "gz"), None, None),
        P(("tx", "ty", "gz"), None),
        P(("tx", "ty", "gz"), None),
        P(("tx", "ty", "gz"), None),
    )
    out_specs = (P("tx", "ty", "gz"), P(("tx", "ty", "gz")))
    return jax.shard_map(update, mesh=mesh, in_specs=in_specs, out_specs=out_specs, check_vma=False)
```
